32 devices in a mesh: sub: 8 (over z, y), slab: 4 (over x, core).
Axes of the slice: x: 2, y: 2, z: 4, core: 2. Of those that a mesh axis runs over, the one named last changes fastest.
Arguments:
- rhs: float32 [8, 64, 8, 512], P(None, 'sub', None, 'slab'), may hold values from -60 to 60, as said below
- perm: float32 [64, 8, 512], P('sub', None, 'slab'), may hold values from 0.1 to 10
- accum: float32 [64, 8, 512], P('sub', None, 'slab'), may hold values from 0.05 to 0.5
- counts: int32 [8], replicated, may hold values from 1 to 8, as said below
Outputs:
- solution: float32 [8, 64, 8, 512], P(None, 'sub', None, 'slab')
- residual: float32 [8, 64, 8, 512], P(None, 'sub', None, 'slab')
The draws below stay inside these ranges and needn't reach their ends.
Inputs may be any that keep to these rules, and one draw needn't show every extreme that they name: `rhs`: pressure sources of the 8 systems; values on planes that are not live are never read. counts[i] live planes fill the first slots of subdomain i; some subdomain has 8.
All inputs are finite; a program needn't handle non-finite values.
Results may differ from the reference program's by a relative error of at most 0.00045.
Values sent between devices are 32-bit elements; how exact they have to be, the bound alone decides.
A program may use at most 64 MiB of HBM per device.

```python
import math
import jax
import jax.numpy as jnp
from jax import lax

CX = 8
CY = 8
S = 8
ITERS = 4
DEG = 4
NXB = 64
NZ = 512
N_SUB = 8


def draw_rhs(key, part):
    shape = (S, NXB, CY, NZ)
    column = 10.0 ** (jnp.arange(S, dtype=jnp.float32) / (S - 1) - 0.5)
    along = 1.0 + 2.0 * jnp.arange(NXB, dtype=jnp.float32) / (NXB - 1)
    noise = jnp.clip(jax.random.normal(key, shape, jnp.float32), -6.0, 6.0)
    return noise * column[:, None, None, None] * along[None, :, None, None]


def draw_counts(key, part):
    first = jax.random.fold_in(key, 11)
    second = jax.random.fold_in(key, 12)
    counts = jax.random.randint(first, (NXB // CX,), 1, CX + 1)
    full = jax.random.randint(second, (), 0, NXB // CX)
    return counts.at[full].set(CX).astype(jnp.int32)


def shard_levels(rng, shape, shards, smallest, largest):
    loudness = 1.0
    for axis_at, parts in shards:
        draws = jax.random.uniform(jax.random.fold_in(jax.random.fold_in(rng, 6), axis_at), (parts,), jnp.float32, smallest / len(shards), largest / len(shards))
        loudness = loudness * jnp.repeat(jnp.exp(draws), shape[axis_at] // parts).reshape((-1,) + (1,) * (len(shape) - 1 - axis_at))
    return loudness


def setup_inputs(seed: int = 0) -> dict:
    streams_of = jax.random.split(jax.random.key(seed), 5)
    return {
        "rhs": draw_rhs(jax.random.fold_in(streams_of[4], 71), 0),
        "perm": jnp.clip(jnp.exp(math.log(10.0) - 4.6051702 * jax.random.uniform(streams_of[1], (NXB, CY, NZ), jnp.float32) ** shard_levels(streams_of[1], (NXB, CY, NZ), ((0, 8), (2, 4)), -0.2, 0.2)), 0.1, 10.0),
        "accum": jnp.clip(jnp.exp(math.log(0.5) - 2.3025851 * jax.random.uniform(streams_of[2], (NXB, CY, NZ), jnp.float32) ** shard_levels(streams_of[2], (NXB, CY, NZ), ((0, 8), (2, 4)), -0.2, 0.2)), 0.05, 0.5),
        "counts": draw_counts(jax.random.fold_in(streams_of[4], 71), 0),
    }


cheb_low = 0.05
cheb_high = 2.0

def neighbours(field, counts):
    rows = field.shape[0]
    grid = field.reshape(rows, N_SUB, CX, CY, NZ)
    plane = lax.broadcasted_iota(jnp.int32, (1, 1, CX, 1, 1), 2)
    live = counts.astype(jnp.int32).reshape(1, N_SUB, 1, 1, 1)
    zero_plane = jnp.zeros_like(grid[:, :, :1])
    up_inside = jnp.concatenate([grid[:, :, 1:], zero_plane], axis=2)
    down_inside = jnp.concatenate([zero_plane, grid[:, :, :-1]], axis=2)
    firsts = grid[:, :, :1]
    after = jnp.concatenate([firsts[:, 1:], jnp.zeros_like(firsts[:, :1])], axis=1)
    lasts = jnp.sum(jnp.where(plane == live - 1, grid, jnp.float32(0.0)), axis=2, keepdims=True)
    before = jnp.concatenate([jnp.zeros_like(lasts[:, :1]), lasts[:, :-1]], axis=1)
    x_next = jnp.where(plane == live - 1, after, up_inside).reshape(field.shape)
    x_prev = jnp.where(plane == 0, before, down_inside).reshape(field.shape)
    zero_row = jnp.zeros_like(field[:, :, :1])
    y_next = jnp.concatenate([field[:, :, 1:], zero_row], axis=2)
    y_prev = jnp.concatenate([zero_row, field[:, :, :-1]], axis=2)
    zero_col = jnp.zeros_like(field[..., :1])
    z_next = jnp.concatenate([field[..., 1:], zero_col], axis=3)
    z_prev = jnp.concatenate([zero_col, field[..., :-1]], axis=3)
    return (x_next, x_prev, y_next, y_prev, z_next, z_prev)

def product(left, right):
    return lax.dot_general(left.reshape(left.shape[0], -1), right.reshape(right.shape[0], -1), (((1,), (1,)), ((), ())), precision=lax.Precision.HIGHEST)

def combine(coef, block):
    flat = jnp.dot(coef, block.reshape(block.shape[0], -1), precision=lax.Precision.HIGHEST)
    return flat.reshape(block.shape)

def lower_solve(factor, block):
    flat = jax.scipy.linalg.solve_triangular(factor, block.reshape(block.shape[0], -1), lower=True)
    return flat.reshape(block.shape)

def precondition(vector, operate, inv_diag):
    theta = 0.5 * (cheb_high + cheb_low)
    delta = 0.5 * (cheb_high - cheb_low)
    sigma = theta / delta
    remain = vector
    update = inv_diag * remain * (1.0 / theta)
    result = update
    rho = 1.0 / sigma
    for step in range(DEG - 1):
        remain = remain - operate(update)
        rho_next = 1.0 / (2.0 * sigma - rho)
        update = rho_next * rho * update + 2.0 * rho_next / delta * (inv_diag * remain)
        result = result + update
        rho = rho_next
    return result

def small_solve(coefs, lowers, lead):
    hess = jnp.zeros((ITERS * S, (ITERS + 1) * S), jnp.float32)
    for j in range(ITERS):
        for i in range(j + 1):
            hess = hess.at[j * S:(j + 1) * S, i * S:(i + 1) * S].set(coefs[j][i])
        hess = hess.at[j * S:(j + 1) * S, (j + 1) * S:(j + 2) * S].set(lowers[j])
    target = jnp.zeros((S, (ITERS + 1) * S), jnp.float32).at[:, :S].set(lead)
    normal = jnp.dot(hess, hess.T, precision=lax.Precision.HIGHEST)
    right = jnp.dot(hess, target.T, precision=lax.Precision.HIGHEST)
    factor = jnp.linalg.cholesky(normal)
    mix = jax.scipy.linalg.cho_solve((factor, True), right).T
    return (mix, hess, target)

def reference(rhs, perm, accum, counts):
    owner = jnp.arange(NXB, dtype=jnp.int32) // CX
    slot = jnp.arange(NXB, dtype=jnp.int32) % CX
    live_planes = (slot < counts.astype(jnp.int32)[owner]).astype(jnp.float32)
    mask = live_planes.reshape(1, NXB, 1, 1)
    field_perm = perm[None]
    near = neighbours(field_perm, counts)
    conduct = []
    diag = accum[None]
    for other in near:
        weight = 2.0 * field_perm * other / (field_perm + other)
        conduct.append(weight)
        diag = diag + weight
    inv_diag = mask / diag

    def operate(field):
        beside = neighbours(field, counts)
        total = diag * field
        for weight, other in zip(conduct, beside):
            total = total - weight * other
        return mask * total
    start = rhs * mask
    lead = jnp.linalg.cholesky(product(start, start))
    basis = [lower_solve(lead, start)]
    coefs = []
    lowers = []
    for step in range(ITERS):
        work = operate(precondition(basis[step], operate, inv_diag))
        found = [product(work, basis[i]) for i in range(step + 1)]
        for i in range(step + 1):
            work = work - combine(found[i], basis[i])
        lower = jnp.linalg.cholesky(product(work, work))
        basis.append(lower_solve(lower, work))
        coefs.append(found)
        lowers.append(lower)
    mix, hess, target = small_solve(coefs, lowers, lead)
    combo = combine(mix[:, :S], basis[0])
    for j in range(1, ITERS):
        combo = combo + combine(mix[:, j * S:(j + 1) * S], basis[j])
    solution = precondition(combo, operate, inv_diag)
    residual = start - operate(solution)
    return (solution, residual)
```

```python
import functools

import jax
import jax.numpy as jnp
from jax import lax
from jax.experimental import pallas as pl
from jax.experimental.pallas import tpu as pltpu
from jax.sharding import PartitionSpec as P

S = 8
ITERS = 4
DEG = 4


cheb_low = 0.05
cheb_high = 2.0


def with_halo(cells, sides, width):
    for axis, dim in sides:
        count = lax.axis_size(axis)
        ends = count - 1
        head = lax.slice_in_dim(cells, 0, width, axis=dim)
        tail = lax.slice_in_dim(cells, cells.shape[dim] - width, cells.shape[dim], axis=dim)
        cells = jnp.concatenate(
            [
                lax.ppermute(tail, axis, [(i, (i + 1) % count) for i in range(ends)]),
                cells,
                lax.ppermute(head, axis, [((i + 1) % count, i) for i in range(ends)]),
            ],
            axis=dim,
        )
    return cells


def neighbours(field, live, plane):
    first = field[:, 0]
    last = lax.dynamic_index_in_dim(field, live - 1, 1, keepdims=False)
    edges = with_halo(jnp.stack([first, last], axis=1), (("sub", 1),), 1)
    before = edges[:, 0:1]
    after = edges[:, 3:4]
    zero_plane = jnp.zeros_like(field[:, :1])
    up_inside = jnp.concatenate([field[:, 1:], zero_plane], axis=1)
    down_inside = jnp.concatenate([zero_plane, field[:, :-1]], axis=1)
    x_next = jnp.where(plane == live - 1, after, up_inside)
    x_prev = jnp.where(plane == 0, before, down_inside)
    zero_row = jnp.zeros_like(field[:, :, :1])
    y_next = jnp.concatenate([field[:, :, 1:], zero_row], axis=2)
    y_prev = jnp.concatenate([zero_row, field[:, :, :-1]], axis=2)
    padded = with_halo(field, (("slab", 3),), 1)
    z_next = padded[..., 2:]
    z_prev = padded[..., :-2]
    return (x_next, x_prev, y_next, y_prev, z_next, z_prev)


def product(left, right):
    return lax.dot_general(
        left.reshape(left.shape[0], -1),
        right.reshape(right.shape[0], -1),
        (((1,), (1,)), ((), ())),
        precision=lax.Precision.HIGHEST,
    )


def combine(coef, block):
    flat = jnp.dot(coef, block.reshape(block.shape[0], -1), precision=lax.Precision.HIGHEST)
    return flat.reshape(block.shape)


def lower_solve(factor, block):
    flat = jax.scipy.linalg.solve_triangular(factor, block.reshape(block.shape[0], -1), lower=True)
    return flat.reshape(block.shape)


def precondition(vector, operate, inv_diag):
    theta = 0.5 * (cheb_high + cheb_low)
    delta = 0.5 * (cheb_high - cheb_low)
    sigma = theta / delta
    remain = vector
    update = inv_diag * remain * (1.0 / theta)
    result = update
    rho = 1.0 / sigma
    for step in range(DEG - 1):
        remain = remain - operate(update)
        rho_next = 1.0 / (2.0 * sigma - rho)
        update = rho_next * rho * update + 2.0 * rho_next / delta * (inv_diag * remain)
        result = result + update
        rho = rho_next
    return result


def small_solve(coefs, lowers, lead):
    hess = jnp.zeros((ITERS * S, (ITERS + 1) * S), jnp.float32)
    for j in range(ITERS):
        for i in range(j + 1):
            hess = hess.at[j * S : (j + 1) * S, i * S : (i + 1) * S].set(coefs[j][i])
        hess = hess.at[j * S : (j + 1) * S, (j + 1) * S : (j + 2) * S].set(lowers[j])
    target = jnp.zeros((S, (ITERS + 1) * S), jnp.float32).at[:, :S].set(lead)
    normal = jnp.dot(hess, hess.T, precision=lax.Precision.HIGHEST)
    right = jnp.dot(hess, target.T, precision=lax.Precision.HIGHEST)
    factor = jnp.linalg.cholesky(normal)
    mix = jax.scipy.linalg.cho_solve((factor, True), right).T
    return (mix, hess, target)


def body(rhs, perm, accum, counts):
    live = counts[lax.axis_index("sub")]
    depth = rhs.shape[1]
    plane = lax.broadcasted_iota(jnp.int32, (1, depth, 1, 1), 1)
    mask = (plane < live).astype(jnp.float32)
    field_perm = perm[None]
    near = neighbours(field_perm, live, plane)
    conduct = []
    diag = accum[None]
    for other in near:
        weight = 2.0 * field_perm * other / (field_perm + other)
        conduct.append(weight)
        diag = diag + weight
    inv_diag = mask / diag

    def operate(field):
        beside = neighbours(field, live, plane)
        total = diag * field
        for weight, other in zip(conduct, beside):
            total = total - weight * other
        return mask * total

    start = rhs * mask
    lead = jnp.linalg.cholesky(lax.psum(product(start, start), ("sub", "slab")))
    basis = [lower_solve(lead, start)]
    coefs = []
    lowers = []
    for step in range(ITERS):
        direction = precondition(basis[step], operate, inv_diag)
        work = operate(direction)
        stacked, whole = lax.psum(
            (jnp.stack([product(work, basis[i]) for i in range(step + 1)]), product(work, work)),
            ("sub", "slab"),
        )
        found = [stacked[i] for i in range(step + 1)]
        block = whole
        for i in range(step + 1):
            work = work - combine(found[i], basis[i])
            block = block - jnp.dot(found[i], found[i].T, precision=lax.Precision.HIGHEST)
        lower = jnp.linalg.cholesky(block)
        basis.append(lower_solve(lower, work))
        coefs.append(found)
        lowers.append(lower)
    mix, hess, target = small_solve(coefs, lowers, lead)
    combo = combine(mix[:, :S], basis[0])
    for j in range(1, ITERS):
        combo = combo + combine(mix[:, j * S : (j + 1) * S], basis[j])
    solution = precondition(combo, operate, inv_diag)
    residual = start - operate(solution)
    return (solution, residual)

LANES = 128


def full(dims, left, right):
    return lax.dot_general(
        left,
        right,
        (dims, ((), ())),
        precision=lax.Precision.HIGHEST,
        preferred_element_type=jnp.float32,
    )


def chebyshev_steps():
    theta = 0.5 * (cheb_high + cheb_low)
    delta = 0.5 * (cheb_high - cheb_low)
    sigma = theta / delta
    rho = 1.0 / sigma
    steps = []
    for _ in range(DEG - 1):
        rho_next = 1.0 / (2.0 * sigma - rho)
        steps.append((rho_next * rho, 2.0 * rho_next / delta))
        rho = rho_next
    return 1.0 / theta, steps


CHUNK = 6


def eliminate(mat, rows, jordan):
    row = lax.broadcasted_iota(jnp.int32, mat.shape, 0)
    for k in range(rows):
        column = jnp.broadcast_to(mat[:, k : k + 1], mat.shape)
        pivot = column[k : k + 1, :]
        line = mat[k : k + 1, :]
        if jordan:
            scaled = line / pivot
            mat = jnp.where(row == k, scaled, mat - column * scaled)
        else:
            root = lax.rsqrt(pivot)
            root = root * (1.5 - 0.5 * pivot * root * root)
            scaled = line * root
            mat = jnp.where(row == k, scaled, jnp.where(row > k, mat - column * root * scaled, mat))
    return mat


SPREAD = 0.52
REACH = 2


def kernel(
    dims,
    rhs_ref, perm_ref, accum_ref, counts_ref, out0_ref, out1_ref,
    pick_ref, raw_ref, out_ref, in_buf, in_got, out_buf, out_got,
    ext, coef, inv, diag_own, basis, big, found, d1, d2, d3, rem,
    part, got1, mid, got2, square, normal,
    in_send, in_recv, out_send, out_recv, xs_send, xs_recv, halo_send, halo_recv, s1_send, s1_recv, s2_send, s2_recv,
):
    nsub, nslab, zl, yl_n, pack, nx = dims
    halo = DEG * REACH
    pad = halo + 1
    span = zl + 2 * halo
    per = yl_n + 1
    sub = lax.axis_index("sub")
    slab = lax.axis_index("slab")

    def position(i):
        across = lax.rem(i, 2)
        at = i // 2 + across * (nsub - 1 - 2 * (i // 2))
        return at + lax.rem(slab, 2) * (nsub - 1 - 2 * at)

    place = slab * nsub + position(sub)
    total = nsub * nslab
    nxt = lax.rem(place + 1, total)
    prv = lax.rem(place + total - 1, total)

    def dev(g):
        at = lax.rem(g, nsub)
        at = at + lax.rem(g // nsub, 2) * (nsub - 1 - 2 * at)
        across = at // (nsub // 2)
        return {"sub": 2 * (at + across * (nsub - 1 - 2 * at)) + across, "slab": g // nsub}

    barrier = pltpu.get_barrier_semaphore()
    for d in range(1, nslab):
        pl.semaphore_signal(
            barrier, inc=1, device_id={"slab": lax.rem(slab + d, nslab)}, device_id_type=pl.DeviceIdType.MESH
        )
    for d in range(1, nsub):
        pl.semaphore_signal(
            barrier, inc=1, device_id={"sub": lax.rem(sub + d, nsub)}, device_id_type=pl.DeviceIdType.MESH
        )
    for g in (nxt, prv):
        pl.semaphore_signal(barrier, inc=1, device_id=dev(g), device_id_type=pl.DeviceIdType.MESH)

    def remote(src, dst, send, recv, device):
        return pltpu.make_async_remote_copy(
            src_ref=src, dst_ref=dst, send_sem=send, recv_sem=recv,
            device_id=device, device_id_type=pl.DeviceIdType.MESH,
        )

    group = pack * (LANES // (pack * nsub))
    pieces = [ref[pl.ds(y, group, stride=yl_n), :] for ref in (perm_ref, accum_ref) for y in range(yl_n)]
    in_buf[yl_n] = jnp.concatenate(pieces, axis=0).T
    for y in range(yl_n):
        in_buf[y] = rhs_ref[pl.ds(y, LANES, stride=yl_n), :].T

    pl.semaphore_wait(barrier, nslab + nsub)

    def rows_of(i):
        return pl.ds(pl.multiple_of(position(i) * zl, 8), zl)

    halves = ((yl_n, 1), (0, yl_n))
    arrivals = []
    for k, (t, n) in enumerate(halves):
        for d in range(1, nsub):
            peer = lax.rem(sub + d, nsub)
            c = remote(
                in_buf.at[t : t + n, rows_of(peer), :], in_got.at[sub, t : t + n],
                in_send.at[k, d], in_recv.at[k, sub], {"sub": peer},
            )
            c.start()
            arrivals.append(c)
    in_got[sub] = in_buf[:, rows_of(sub), :]

    def arrived(k):
        t, n = halves[k]
        for d in range(1, nsub):
            peer = lax.rem(sub + d, nsub)
            remote(
                in_buf.at[t : t + n, rows_of(peer), :], in_got.at[peer, t : t + n],
                in_send.at[k, d], in_recv.at[k, peer], {"sub": peer},
            ).wait_recv()

    wide_row = lax.broadcasted_iota(jnp.int32, (LANES, LANES), 0)
    wide_lane = lax.broadcasted_iota(jnp.int32, (LANES, LANES), 1)
    rank = lax.rem(wide_row, group) // pack
    owner = wide_row // group
    base_of = jnp.zeros_like(wide_row)
    live_of = jnp.zeros_like(wide_row)
    before = jnp.int32(0)
    for i in range(nsub):
        live = counts_ref[i]
        base_of = jnp.where(owner == i, before, base_of)
        live_of = jnp.where(owner == i, live, live_of)
        before = before + live
    goal = base_of + rank + lax.rem(wide_row, pack) * nx
    pick_ref[...] = jnp.where((rank < live_of) & (goal == wide_lane), 1.0, 0.0).astype(jnp.float32)
    square[...] = jnp.zeros_like(square)

    strip = lax.broadcasted_iota(jnp.int32, (zl, LANES), 1) // group

    def butterfly(items):
        d = len(items) // 2
        while d:
            fresh = list(items)
            for a in range(len(items)):
                if a & d:
                    continue
                first_half = (strip & d) == 0
                fresh[a] = jnp.where(first_half, items[a], pltpu.roll(items[a + d], group * d, 1))
                fresh[a + d] = jnp.where(first_half, pltpu.roll(items[a], LANES - group * d, 1), items[a + d])
            items = fresh
            d //= 2
        return items

    lane = lax.broadcasted_iota(jnp.int32, (8, LANES), 1)
    row = lax.broadcasted_iota(jnp.int32, (8, LANES), 0)
    tile = yl_n * LANES
    side = halo * tile
    own_lo, own_hi = side, side + zl * tile

    arrived(0)
    for i, value in enumerate(butterfly([in_got[i, yl_n] for i in range(nsub)])):
        raw_ref[pl.ds(i, zl, stride=8), :] = value
    packed = full(((1,), (0,)), raw_ref[0 : zl * 8, :], pick_ref[...])
    for k in range(zl):
        at = (pad + k) * LANES
        ext[:, at : at + LANES] = packed[k * 8 : k * 8 + 8, :]
    edge = pad * LANES
    whole = zl * LANES
    up = remote(ext.at[:, whole : whole + edge], ext.at[:, 0:edge], xs_send.at[0], xs_recv.at[0], dev(nxt))
    down = remote(ext.at[:, edge : 2 * edge], ext.at[:, edge + whole : 2 * edge + whole], xs_send.at[1], xs_recv.at[1], dev(prv))
    up.start()
    down.start()

    arrived(1)
    for t in range(yl_n):
        for i, value in enumerate(butterfly([in_got[i, t] for i in range(nsub)])):
            raw_ref[pl.ds(t * 8 + i, zl, stride=yl_n * 8), :] = value
    packed = full(((1,), (0,)), raw_ref[...], pick_ref[...])
    for k in range(zl * yl_n):
        basis[0, :, own_lo + k * LANES : own_lo + (k + 1) * LANES] = packed[k * 8 : k * 8 + 8, :]
        big[0:8, k * LANES : (k + 1) * LANES] = packed[k * 8 : k * 8 + 8, :]

    def swap(n, m):
        return [
            remote(
                basis.at[n, :, own_hi - side : own_hi], basis.at[n, :, 0:side],
                halo_send.at[m, 0], halo_recv.at[m, 0], dev(nxt),
            ),
            remote(
                basis.at[n, :, own_lo : own_lo + side], basis.at[n, :, own_hi : own_hi + side],
                halo_send.at[m, 1], halo_recv.at[m, 1], dev(prv),
            ),
        ]

    first_swap = swap(0, 0)
    for c in first_swap:
        c.start()

    def products(j):
        blocks = j + 1

        def add(k, accs):
            accs = list(accs)
            for h in range(2):
                at = pl.ds(pl.multiple_of((2 * k + h) * LANES, LANES), LANES)
                w = big[8 * j : 8 * j + 8, at]
                turned = [w] + [pltpu.roll(w, n, 0) for n in range(1, 8)]
                for b in range(blocks):
                    v = w if b == j else big[8 * b : 8 * b + 8, at]
                    for n in range(8):
                        accs[8 * b + n] = accs[8 * b + n] + v * turned[n]
            return tuple(accs)

        zero = jnp.zeros((8, LANES), jnp.float32)
        accs = lax.fori_loop(0, zl * yl_n // 2, add, (zero,) * (8 * blocks))
        out = zero
        for b in range(blocks):
            for n in range(8):
                acc = accs[8 * b + n]
                acc = pltpu.roll(acc, 8 - n, 0) if n else acc
                line = jnp.sum(acc, axis=1, keepdims=True)
                out = jnp.where(lane == 8 * b + lax.rem(row + n, 8), line, out)
        return out

    sends = []

    def reduce_begin(r, gram):
        part[r] = gram
        got1[r, slab] = part[r]
        for d in range(1, nslab):
            peer = lax.rem(slab + d, nslab)
            c = remote(part.at[r], got1.at[r, slab], s1_send.at[r, d], s1_recv.at[r, slab], {"slab": peer})
            c.start()
            sends.append(c)

    def reduce_middle(r):
        for d in range(1, nslab):
            peer = lax.rem(slab + d, nslab)
            remote(part.at[r], got1.at[r, peer], s1_send.at[r, d], s1_recv.at[r, peer], {"slab": peer}).wait_recv()
        acc = got1[r, 0]
        for i in range(1, nslab):
            acc = acc + got1[r, i]
        mid[r] = acc
        got2[r, sub] = acc
        for d in range(1, nsub):
            peer = lax.rem(sub + d, nsub)
            c = remote(mid.at[r], got2.at[r, sub], s2_send.at[r, d], s2_recv.at[r, sub], {"sub": peer})
            c.start()
            sends.append(c)

    def reduce_end(r):
        for d in range(1, nsub):
            peer = lax.rem(sub + d, nsub)
            remote(mid.at[r], got2.at[r, peer], s2_send.at[r, d], s2_recv.at[r, peer], {"sub": peer}).wait_recv()
        acc = got2[r, 0]
        for i in range(1, nsub):
            acc = acc + got2[r, i]
        return acc

    up.wait()
    down.wait()
    low = jnp.where(place == 0, 0.0, 1.0).astype(jnp.float32)
    high = jnp.where(place == total - 1, 0.0, 1.0).astype(jnp.float32)
    for k in range(pad):
        a = k * LANES
        ext[:, a : a + LANES] = ext[:, a : a + LANES] * low
        b = (pad + zl + k) * LANES
        ext[:, b : b + LANES] = ext[:, b : b + LANES] * high
    along = lax.rem(lane, nx)

    def fill(e, _):
        def grab(t):
            return ext[:, pl.ds(pl.multiple_of((e + 1 + t) * LANES, LANES), LANES)]

        here, after, before = grab(0), grab(1), grab(-1)
        swap_up = pltpu.roll(here, LANES - nx, 1)
        swap_down = pltpu.roll(here, nx, 1)
        x_up = jnp.where(along == nx - 1, 0.0, pltpu.roll(here, LANES - 1, 1))
        x_down = jnp.where(along == 0, 0.0, pltpu.roll(here, 1, 1))
        swap_up = jnp.where(lane >= LANES - nx, 0.0, swap_up)
        swap_down = jnp.where(lane < nx, 0.0, swap_down)

        def line(value, y):
            return jnp.broadcast_to(value[y : y + 1, :], (8, LANES))

        for y in range(yl_n):
            p = line(here, y)
            others = (
                line(x_up, y),
                line(x_down, y),
                line(here, y + 1) if y + 1 < yl_n else line(swap_up, 0),
                line(here, y - 1) if y > 0 else line(swap_down, yl_n - 1),
                line(after, y),
                line(before, y),
            )
            at = pl.ds(pl.multiple_of((e * yl_n + y) * LANES, LANES), LANES)
            diag = line(here, yl_n + y)
            weights = []
            for q in others:
                both = p * q
                weight = jnp.where(both > 0.0, 2.0 * both / jnp.where(both > 0.0, p + q, 1.0), 0.0)
                weights.append(weight)
                diag = diag + weight
            over = jnp.where(diag > 0.0, 1.0 / jnp.where(diag > 0.0, diag, 1.0), 0.0)
            for k, weight in enumerate(weights):
                coef[k, :, at] = weight * over
            inv[:, at] = over
            diag_own[:, at] = diag
        return 0

    lax.fori_loop(0, span, fill, 0)

    reduce_begin(0, products(0))
    for c in first_swap:
        c.wait()

    def scale(k, _):
        for h in range(yl_n):
            at = pl.ds(pl.multiple_of((k * yl_n + h) * LANES, LANES), LANES)
            basis[0, :, at] = basis[0, :, at] * inv[:, at]
        return 0

    lax.fori_loop(0, span, scale, 0)

    first, steps = chebyshev_steps()

    def spot(e, y):
        if isinstance(e, int):
            return pl.ds((e * yl_n + y) * LANES, LANES)
        return pl.ds(pl.multiple_of((e * yl_n + y) * LANES, LANES), LANES)

    def beside(field, e):
        here = [field[:, spot(e, y)] for y in range(yl_n)]
        outs = []
        for y in range(yl_n):
            at = spot(e, y)
            f = here[y]
            y_up = here[y + 1] if y + 1 < yl_n else pltpu.roll(here[0], LANES - nx, 1)
            y_down = here[y - 1] if y > 0 else pltpu.roll(here[yl_n - 1], nx, 1)
            acc = coef[0, :, at] * pltpu.roll(f, LANES - 1, 1)
            acc = acc + coef[1, :, at] * pltpu.roll(f, 1, 1)
            acc = acc + coef[2, :, at] * y_up
            acc = acc + coef[3, :, at] * y_down
            acc = acc + coef[4, :, at] * field[:, spot(e + 1, y)]
            acc = acc + coef[5, :, at] * field[:, spot(e - 1, y)]
            outs.append(acc)
        return here, outs

    def sweep(lo, hi, work, chunk=CHUNK):
        turns = (hi - lo) // chunk

        def one(k, _):
            work([lo + k * chunk + n for n in range(chunk)])
            return 0

        if turns > 1:
            lax.fori_loop(0, turns, one, 0)
        elif turns:
            work(list(range(lo, lo + chunk)))
        if lo + turns * chunk < hi:
            work(list(range(lo + turns * chunk, hi)))

    def advance(j):
        start = basis.at[j]
        inset = DEG * (j % REACH)
        fields = (start, d1, d2, d3)
        for t, (keep, gain) in enumerate(steps):
            def one(es, t=t, keep=keep, gain=gain):
                source, target = fields[t], fields[t + 1]
                for e in es:
                    here, outs = beside(source, e)
                    for y in range(yl_n):
                        at = spot(e, y)
                        if t == 0:
                            r = here[y] - first * (here[y] - outs[y])
                            d = (keep * first) * here[y] + gain * r
                        else:
                            r = rem[:, at] - here[y] + outs[y]
                            d = keep * here[y] + gain * r
                        rem[:, at] = r
                        target[:, at] = d

            sweep(inset + t + 1, span - inset - t - 1, one)

        def last(es, own):
            for e in es:
                here, outs = beside(d3, e)
                for y in range(yl_n):
                    at = spot(e, y)
                    r = rem[:, at] - here[y] + outs[y]
                    value = r * (1.0 / SPREAD) if j == 0 else r * (2.0 / SPREAD) - basis[j - 1, :, at]
                    if j + 1 < ITERS:
                        basis[j + 1, :, at] = value
                    if own:
                        to = spot(e - halo, y)
                        big[8 * (j + 1) : 8 * (j + 2), to] = value * diag_own[:, at]
                        found[8 * j : 8 * (j + 1), to] = first * start[:, at] + d1[:, at] + d2[:, at] + here[y]

        if inset + DEG < halo:
            sweep(inset + DEG, halo, lambda es: last(es, False))
            sweep(halo + zl, span - inset - DEG, lambda es: last(es, False))
        sweep(halo, halo + zl, lambda es: last(es, True))

    for j in range(ITERS):
        advance(j)
        moves = []
        if (j + 1) % REACH == 0 and j + 1 < ITERS:
            moves = swap(j + 1, (j + 1) // REACH)
            for c in moves:
                c.start()
        reduce_begin(j + 1, products(j + 1))
        reduce_middle(j)
        for c in moves:
            c.wait()
    reduce_middle(ITERS)

    rows = 8 * ITERS
    for r in range(ITERS + 1):
        square[8 * r : 8 * r + 8, :] = reduce_end(r)
    turned = square[...].T
    gram = [
        jnp.where(lane < 8 * (r + 1), square[8 * r : 8 * r + 8, :], turned[8 * r : 8 * r + 8, :])
        for r in range(ITERS + 1)
    ]
    up_by = jnp.where(lane < 8, SPREAD, 0.5 * SPREAD)
    down_by = jnp.where(lane < 8, 0.0, 0.5 * SPREAD)
    for j in range(ITERS):
        mixed = gram[j] - SPREAD * gram[1] if j == 0 else gram[j] - (0.5 * SPREAD) * (gram[j + 1] + gram[j - 1])
        both = mixed - up_by * pltpu.roll(mixed, LANES - 8, 1) - down_by * pltpu.roll(mixed, 8, 1)
        right = pltpu.roll(mixed, rows, 1)
        normal[8 * j : 8 * j + 8, :] = jnp.where(lane < rows, both, jnp.where(lane < rows + 8, right, 0.0))
    solved = eliminate(normal[...], rows, True)
    filled = jnp.concatenate([solved, jnp.zeros((LANES - rows, LANES), jnp.float32)], axis=0)
    mix = filled.T[rows : rows + 8, :]
    used = mix - pltpu.roll(mix * up_by, 8, 1) - pltpu.roll(mix * down_by, LANES - 8, 1)
    answer = full(((1,), (0,)), mix[:, 0:rows], found[...])
    taken = full(((1,), (0,)), used[:, 0 : rows + 8], big[...])
    for k in range(zl * yl_n):
        at = slice(k * LANES, (k + 1) * LANES)
        out_ref[0, k * 8 : k * 8 + 8, :] = answer[:, at]
        out_ref[1, k * 8 : k * 8 + 8, :] = big[0:8, at] - taken[:, at]

    for f in range(2):
        raw_ref[...] = full(((1,), (1,)), out_ref[f], pick_ref[...])
        for y in range(yl_n):
            items = [raw_ref[pl.ds(y * 8 + i, zl, stride=yl_n * 8), :] for i in range(nsub)]
            for i, value in enumerate(butterfly(items)):
                out_buf[i, f * yl_n + y] = value
    leaving = []
    for d in range(1, nsub):
        peer = lax.rem(sub + d, nsub)
        c = remote(out_buf.at[peer], out_got.at[:, rows_of(sub), :], out_send.at[d], out_recv.at[sub], {"sub": peer})
        c.start()
        leaving.append(c)
    out_got[:, rows_of(sub), :] = out_buf[sub]
    for d in range(1, nsub):
        peer = lax.rem(sub + d, nsub)
        remote(out_buf.at[peer], out_got.at[:, rows_of(peer), :], out_send.at[d], out_recv.at[peer], {"sub": peer}).wait_recv()
    for f, ref in enumerate((out0_ref, out1_ref)):
        for y in range(yl_n):
            ref[pl.ds(y, LANES, stride=yl_n), :] = out_got[f * yl_n + y].T
    for c in arrivals + leaving + sends:
        c.wait_send()


def fast_body(rhs, perm, accum, counts):
    nsub, nslab = lax.axis_size("sub"), lax.axis_size("slab")
    s, depth, cy, zs = rhs.shape
    nx = depth * nsub
    pack = LANES // nx
    yl = cy // pack
    zl = zs // nsub
    halo = DEG * REACH
    span = zl + 2 * halo
    pad = halo + 1

    wide = span * yl * LANES
    own = zl * yl * LANES
    f32 = jnp.float32
    rounds = ITERS + 1
    dma = pltpu.SemaphoreType.DMA
    out = pl.pallas_call(
        functools.partial(kernel, (nsub, nslab, zl, yl, pack, nx)),
        out_shape=[jax.ShapeDtypeStruct((s * depth * cy, zs), f32)] * 2,
        in_specs=[pl.BlockSpec(memory_space=pltpu.VMEM)] * 3 + [pl.BlockSpec(memory_space=pltpu.SMEM)],
        out_specs=[pl.BlockSpec(memory_space=pltpu.VMEM)] * 2,
        scratch_shapes=[
            pltpu.VMEM((LANES, LANES), f32),
            pltpu.VMEM((zl * yl * s, LANES), f32),
            pltpu.VMEM((2, zl * yl * s, LANES), f32),
            pltpu.VMEM((yl + 1, zs, LANES), f32),
            pltpu.VMEM((nsub, yl + 1, zl, LANES), f32),
            pltpu.VMEM((nsub, 2 * yl, zl, LANES), f32),
            pltpu.VMEM((2 * yl, zs, LANES), f32),
            pltpu.VMEM((8, (zl + 2 * pad) * LANES), f32),
            pltpu.VMEM((6, 8, wide), f32),
            pltpu.VMEM((8, wide), f32),
            pltpu.VMEM((8, wide), f32),
            pltpu.VMEM((ITERS, 8, wide), f32),
            pltpu.VMEM((8 * rounds, own), f32),
            pltpu.VMEM((8 * ITERS, own), f32),
            pltpu.VMEM((8, wide), f32),
            pltpu.VMEM((8, wide), f32),
            pltpu.VMEM((8, wide), f32),
            pltpu.VMEM((8, wide), f32),
            pltpu.VMEM((rounds, 8, LANES), f32),
            pltpu.VMEM((rounds, nslab, 8, LANES), f32),
            pltpu.VMEM((rounds, 8, LANES), f32),
            pltpu.VMEM((rounds, nsub, 8, LANES), f32),
            pltpu.VMEM((LANES, LANES), f32),
            pltpu.VMEM((8 * ITERS, LANES), f32),
            dma((2, nsub)),
            dma((2, nsub)),
            dma((nsub,)),
            dma((nsub,)),
            dma((2,)),
            dma((2,)),
            dma((ITERS // REACH, 2)),
            dma((ITERS // REACH, 2)),
            dma((rounds, nslab)),
            dma((rounds, nslab)),
            dma((rounds, nsub)),
            dma((rounds, nsub)),
        ],
        compiler_params=pltpu.CompilerParams(
            collective_id=0, has_side_effects=True, vmem_limit_bytes=48 * 1024 * 1024
        ),
    )(rhs.reshape(-1, zs), perm.reshape(-1, zs), accum.reshape(-1, zs), counts)
    return out[0].reshape(rhs.shape), out[1].reshape(rhs.shape)


def choose(rhs, perm, accum, counts):
    nsub = lax.axis_size("sub")
    s, depth, cy, zs = rhs.shape
    nx = depth * nsub
    fits = s == S == nsub == 8 and zs == LANES and zs // nsub % 8 == 0 and LANES % nx == 0 and zs % nsub == 0 and zs // nsub > DEG * REACH
    fits = fits and cy % max(LANES // nx, 1) == 0 and cy // max(LANES // nx, 1) == 4
    if fits:
        return fast_body(rhs, perm, accum, counts)
    return body(rhs, perm, accum, counts)


def solution(mesh):
    placed = (P(None, "sub", None, "slab"), P("sub", None, "slab"), P("sub", None, "slab"), P())
    return jax.shard_map(
        choose,
        mesh=mesh,
        in_specs=placed,
        out_specs=(P(None, "sub", None, "slab"), P(None, "sub", None, "slab")),
        check_vma=False,
    )
```

```python
import functools

import jax
import jax.numpy as jnp
from jax import lax
from jax.experimental import pallas as pl
from jax.experimental.pallas import tpu as pltpu
from jax.sharding import PartitionSpec as P

S = 8
ITERS = 4
DEG = 4


cheb_low = 0.05
cheb_high = 2.0


def with_halo(cells, sides, width):
    for axis, dim in sides:
        count = lax.axis_size(axis)
        ends = count - 1
        head = lax.slice_in_dim(cells, 0, width, axis=dim)
        tail = lax.slice_in_dim(cells, cells.shape[dim] - width, cells.shape[dim], axis=dim)
        cells = jnp.concatenate(
            [
                lax.ppermute(tail, axis, [(i, (i + 1) % count) for i in range(ends)]),
                cells,
                lax.ppermute(head, axis, [((i + 1) % count, i) for i in range(ends)]),
            ],
            axis=dim,
        )
    return cells


def neighbours(field, live, plane):
    first = field[:, 0]
    last = lax.dynamic_index_in_dim(field, live - 1, 1, keepdims=False)
    edges = with_halo(jnp.stack([first, last], axis=1), (("sub", 1),), 1)
    before = edges[:, 0:1]
    after = edges[:, 3:4]
    zero_plane = jnp.zeros_like(field[:, :1])
    up_inside = jnp.concatenate([field[:, 1:], zero_plane], axis=1)
    down_inside = jnp.concatenate([zero_plane, field[:, :-1]], axis=1)
    x_next = jnp.where(plane == live - 1, after, up_inside)
    x_prev = jnp.where(plane == 0, before, down_inside)
    zero_row = jnp.zeros_like(field[:, :, :1])
    y_next = jnp.concatenate([field[:, :, 1:], zero_row], axis=2)
    y_prev = jnp.concatenate([zero_row, field[:, :, :-1]], axis=2)
    padded = with_halo(field, (("slab", 3),), 1)
    z_next = padded[..., 2:]
    z_prev = padded[..., :-2]
    return (x_next, x_prev, y_next, y_prev, z_next, z_prev)


def product(left, right):
    return lax.dot_general(
        left.reshape(left.shape[0], -1),
        right.reshape(right.shape[0], -1),
        (((1,), (1,)), ((), ())),
        precision=lax.Precision.HIGHEST,
    )


def combine(coef, block):
    flat = jnp.dot(coef, block.reshape(block.shape[0], -1), precision=lax.Precision.HIGHEST)
    return flat.reshape(block.shape)


def lower_solve(factor, block):
    flat = jax.scipy.linalg.solve_triangular(factor, block.reshape(block.shape[0], -1), lower=True)
    return flat.reshape(block.shape)


def precondition(vector, operate, inv_diag):
    theta = 0.5 * (cheb_high + cheb_low)
    delta = 0.5 * (cheb_high - cheb_low)
    sigma = theta / delta
    remain = vector
    update = inv_diag * remain * (1.0 / theta)
    result = update
    rho = 1.0 / sigma
    for step in range(DEG - 1):
        remain = remain - operate(update)
        rho_next = 1.0 / (2.0 * sigma - rho)
        update = rho_next * rho * update + 2.0 * rho_next / delta * (inv_diag * remain)
        result = result + update
        rho = rho_next
    return result


def small_solve(coefs, lowers, lead):
    hess = jnp.zeros((ITERS * S, (ITERS + 1) * S), jnp.float32)
    for j in range(ITERS):
        for i in range(j + 1):
            hess = hess.at[j * S : (j + 1) * S, i * S : (i + 1) * S].set(coefs[j][i])
        hess = hess.at[j * S : (j + 1) * S, (j + 1) * S : (j + 2) * S].set(lowers[j])
    target = jnp.zeros((S, (ITERS + 1) * S), jnp.float32).at[:, :S].set(lead)
    normal = jnp.dot(hess, hess.T, precision=lax.Precision.HIGHEST)
    right = jnp.dot(hess, target.T, precision=lax.Precision.HIGHEST)
    factor = jnp.linalg.cholesky(normal)
    mix = jax.scipy.linalg.cho_solve((factor, True), right).T
    return (mix, hess, target)


def body(rhs, perm, accum, counts):
    live = counts[lax.axis_index("sub")]
    depth = rhs.shape[1]
    plane = lax.broadcasted_iota(jnp.int32, (1, depth, 1, 1), 1)
    mask = (plane < live).astype(jnp.float32)
    field_perm = perm[None]
    near = neighbours(field_perm, live, plane)
    conduct = []
    diag = accum[None]
    for other in near:
        weight = 2.0 * field_perm * other / (field_perm + other)
        conduct.append(weight)
        diag = diag + weight
    inv_diag = mask / diag

    def operate(field):
        beside = neighbours(field, live, plane)
        total = diag * field
        for weight, other in zip(conduct, beside):
            total = total - weight * other
        return mask * total

    start = rhs * mask
    lead = jnp.linalg.cholesky(lax.psum(product(start, start), ("sub", "slab")))
    basis = [lower_solve(lead, start)]
    coefs = []
    lowers = []
    for step in range(ITERS):
        direction = precondition(basis[step], operate, inv_diag)
        work = operate(direction)
        stacked, whole = lax.psum(
            (jnp.stack([product(work, basis[i]) for i in range(step + 1)]), product(work, work)),
            ("sub", "slab"),
        )
        found = [stacked[i] for i in range(step + 1)]
        block = whole
        for i in range(step + 1):
            work = work - combine(found[i], basis[i])
            block = block - jnp.dot(found[i], found[i].T, precision=lax.Precision.HIGHEST)
        lower = jnp.linalg.cholesky(block)
        basis.append(lower_solve(lower, work))
        coefs.append(found)
        lowers.append(lower)
    mix, hess, target = small_solve(coefs, lowers, lead)
    combo = combine(mix[:, :S], basis[0])
    for j in range(1, ITERS):
        combo = combo + combine(mix[:, j * S : (j + 1) * S], basis[j])
    solution = precondition(combo, operate, inv_diag)
    residual = start - operate(solution)
    return (solution, residual)

LANES = 128


def full(dims, left, right):
    return lax.dot_general(
        left,
        right,
        (dims, ((), ())),
        precision=lax.Precision.HIGHEST,
        preferred_element_type=jnp.float32,
    )


def chebyshev_steps():
    theta = 0.5 * (cheb_high + cheb_low)
    delta = 0.5 * (cheb_high - cheb_low)
    sigma = theta / delta
    rho = 1.0 / sigma
    steps = []
    for _ in range(DEG - 1):
        rho_next = 1.0 / (2.0 * sigma - rho)
        steps.append((rho_next * rho, 2.0 * rho_next / delta))
        rho = rho_next
    return 1.0 / theta, steps


def spread_rows(value, k):
    return jnp.broadcast_to(value[k : k + 1, :], value.shape)


def spread_lane(value, k):
    return jnp.broadcast_to(value[:, k : k + 1], value.shape)


def times(columns, block):
    total = columns[0] * spread_rows(block, 0)
    for c in range(1, 8):
        total = total + columns[c] * spread_rows(block, c)
    return total


def invert(cols, row):
    cols = list(cols)
    for k in range(8):
        over = 1.0 / spread_rows(cols[k], k)
        pivot = cols[k]
        for c in range(8):
            if c == k:
                cols[c] = jnp.where(row == k, over, -pivot * over)
            else:
                scaled = spread_rows(cols[c], k) * over
                cols[c] = jnp.where(row == k, scaled, cols[c] - pivot * scaled)
    return cols


def block_jordan(blocks, row):
    blocks = list(blocks)
    for k in range(len(blocks)):
        cols = [[spread_lane(b, 8 * k + c) for c in range(8)] for b in blocks]
        solved = times(invert(cols[k], row), blocks[k])
        for i in range(len(blocks)):
            blocks[i] = solved if i == k else blocks[i] - times(cols[i], solved)
    return blocks


SPREAD = 0.52
REACH = 2


def kernel(
    dims,
    rhs_hbm, perm_hbm, accum_hbm, counts_hbm, out0_ref, out1_ref,
    rhs_ref, perm_ref, accum_ref, counts_ref, load_sem,
    pick_ref, raw_ref, out_ref, in_buf, in_got, out_buf, out_got,
    ext, coef, inv, diag_own, first_field, basis, big, found, d1, d2, d3, rem,
    part, got1, mid, got2, square,
    in_send, in_recv, out_send, out_recv, xs_send, xs_recv, halo_send, halo_recv, s1_send, s1_recv, s2_send, s2_recv,
):
    nsub, nslab, zl, yl_n, pack, nx = dims
    halo = DEG * REACH
    pad = halo + 1
    span = zl + 2 * halo
    per = yl_n + 1
    sub = lax.axis_index("sub")
    slab = lax.axis_index("slab")

    def position(i):
        across = lax.rem(i, 2)
        at = i // 2 + across * (nsub - 1 - 2 * (i // 2))
        return at + lax.rem(slab, 2) * (nsub - 1 - 2 * at)

    place = slab * nsub + position(sub)
    total = nsub * nslab
    nxt = lax.rem(place + 1, total)
    prv = lax.rem(place + total - 1, total)

    def dev(g):
        at = lax.rem(g, nsub)
        at = at + lax.rem(g // nsub, 2) * (nsub - 1 - 2 * at)
        across = at // (nsub // 2)
        return {"sub": 2 * (at + across * (nsub - 1 - 2 * at)) + across, "slab": g // nsub}

    loads = [
        pltpu.make_async_copy(src, dst, load_sem.at[k])
        for k, (src, dst) in enumerate(
            ((perm_hbm, perm_ref), (accum_hbm, accum_ref), (rhs_hbm, rhs_ref), (counts_hbm, counts_ref))
        )
    ]
    for c in loads:
        c.start()

    barrier = pltpu.get_barrier_semaphore()
    for d in range(1, nslab):
        pl.semaphore_signal(
            barrier, inc=1, device_id={"slab": lax.rem(slab + d, nslab)}, device_id_type=pl.DeviceIdType.MESH
        )
    for d in range(1, nsub):
        pl.semaphore_signal(
            barrier, inc=1, device_id={"sub": lax.rem(sub + d, nsub)}, device_id_type=pl.DeviceIdType.MESH
        )
    for g in (nxt, prv):
        pl.semaphore_signal(barrier, inc=1, device_id=dev(g), device_id_type=pl.DeviceIdType.MESH)

    def remote(src, dst, send, recv, device):
        return pltpu.make_async_remote_copy(
            src_ref=src, dst_ref=dst, send_sem=send, recv_sem=recv,
            device_id=device, device_id_type=pl.DeviceIdType.MESH,
        )

    group = pack * (LANES // (pack * nsub))
    square[...] = jnp.zeros_like(square)
    for c in loads:
        c.wait()
    pieces = [ref[pl.ds(y, group, stride=yl_n), :] for ref in (perm_ref, accum_ref) for y in range(yl_n)]
    in_buf[yl_n] = jnp.concatenate(pieces, axis=0).T
    for y in range(yl_n):
        in_buf[y] = rhs_ref[pl.ds(y, LANES, stride=yl_n), :].T

    pl.semaphore_wait(barrier, nslab + nsub)

    def rows_of(i):
        return pl.ds(pl.multiple_of(position(i) * zl, 8), zl)

    halves = ((yl_n, 1), (0, yl_n))
    arrivals = []
    for k, (t, n) in enumerate(halves):
        for d in range(1, nsub):
            peer = lax.rem(sub + d, nsub)
            c = remote(
                in_buf.at[t : t + n, rows_of(peer), :], in_got.at[sub, t : t + n],
                in_send.at[k, d], in_recv.at[k, sub], {"sub": peer},
            )
            c.start()
            arrivals.append(c)
    in_got[sub] = in_buf[:, rows_of(sub), :]

    def arrived(k):
        t, n = halves[k]
        for d in range(1, nsub):
            peer = lax.rem(sub + d, nsub)
            remote(
                in_buf.at[t : t + n, rows_of(peer), :], in_got.at[peer, t : t + n],
                in_send.at[k, d], in_recv.at[k, peer], {"sub": peer},
            ).wait_recv()

    wide_row = lax.broadcasted_iota(jnp.int32, (LANES, LANES), 0)
    wide_lane = lax.broadcasted_iota(jnp.int32, (LANES, LANES), 1)
    rank = lax.rem(wide_row, group) // pack
    owner = wide_row // group
    base_of = jnp.zeros_like(wide_row)
    live_of = jnp.zeros_like(wide_row)
    before = jnp.int32(0)
    for i in range(nsub):
        live = counts_ref[i]
        base_of = jnp.where(owner == i, before, base_of)
        live_of = jnp.where(owner == i, live, live_of)
        before = before + live
    goal = base_of + rank + lax.rem(wide_row, pack) * nx
    pick_ref[...] = jnp.where((rank < live_of) & (goal == wide_lane), 1.0, 0.0).astype(jnp.float32)

    strip = lax.broadcasted_iota(jnp.int32, (zl, LANES), 1) // group

    def butterfly(items):
        d = len(items) // 2
        while d:
            fresh = list(items)
            for a in range(len(items)):
                if a & d:
                    continue
                first_half = (strip & d) == 0
                fresh[a] = jnp.where(first_half, items[a], pltpu.roll(items[a + d], group * d, 1))
                fresh[a + d] = jnp.where(first_half, pltpu.roll(items[a], LANES - group * d, 1), items[a + d])
            items = fresh
            d //= 2
        return items

    lane = lax.broadcasted_iota(jnp.int32, (8, LANES), 1)
    row = lax.broadcasted_iota(jnp.int32, (8, LANES), 0)
    tile = yl_n * LANES
    side = halo * tile
    own_lo, own_hi = side, side + zl * tile

    arrived(0)
    for i, value in enumerate(butterfly([in_got[i, yl_n] for i in range(nsub)])):
        raw_ref[pl.ds(i, zl, stride=8), :] = value
    packed = full(((1,), (0,)), raw_ref[0 : zl * 8, :], pick_ref[...])
    for k in range(zl):
        at = (pad + k) * LANES
        ext[:, at : at + LANES] = packed[k * 8 : k * 8 + 8, :]
    edge = pad * LANES
    whole = zl * LANES
    up = remote(ext.at[:, whole : whole + edge], ext.at[:, 0:edge], xs_send.at[0], xs_recv.at[0], dev(nxt))
    down = remote(ext.at[:, edge : 2 * edge], ext.at[:, edge + whole : 2 * edge + whole], xs_send.at[1], xs_recv.at[1], dev(prv))
    up.start()
    down.start()

    arrived(1)
    for t in range(yl_n):
        for i, value in enumerate(butterfly([in_got[i, t] for i in range(nsub)])):
            raw_ref[pl.ds(t * 8 + i, zl, stride=yl_n * 8), :] = value
    packed = full(((1,), (0,)), raw_ref[...], pick_ref[...])
    for k in range(zl * yl_n):
        basis[0, :, own_lo + k * LANES : own_lo + (k + 1) * LANES] = packed[k * 8 : k * 8 + 8, :]
        big[0:8, k * LANES : (k + 1) * LANES] = packed[k * 8 : k * 8 + 8, :]

    def swap(n, m):
        return [
            remote(
                basis.at[n, :, own_hi - side : own_hi], basis.at[n, :, 0:side],
                halo_send.at[m, 0], halo_recv.at[m, 0], dev(nxt),
            ),
            remote(
                basis.at[n, :, own_lo : own_lo + side], basis.at[n, :, own_hi : own_hi + side],
                halo_send.at[m, 1], halo_recv.at[m, 1], dev(prv),
            ),
        ]

    first_swap = swap(0, 0)
    for c in first_swap:
        c.start()

    def products(j):
        blocks = j + 1

        def add(k, accs):
            accs = list(accs)
            for h in range(2):
                at = pl.ds(pl.multiple_of((2 * k + h) * LANES, LANES), LANES)
                w = big[8 * j : 8 * j + 8, at]
                turned = [w] + [pltpu.roll(w, n, 0) for n in range(1, 8)]
                for b in range(blocks):
                    v = w if b == j else big[8 * b : 8 * b + 8, at]
                    for n in range(8):
                        accs[8 * b + n] = accs[8 * b + n] + v * turned[n]
            return tuple(accs)

        zero = jnp.zeros((8, LANES), jnp.float32)
        accs = lax.fori_loop(0, zl * yl_n // 2, add, (zero,) * (8 * blocks))
        out = zero
        for b in range(blocks):
            for n in range(8):
                acc = accs[8 * b + n]
                acc = pltpu.roll(acc, 8 - n, 0) if n else acc
                line = jnp.sum(acc, axis=1, keepdims=True)
                out = jnp.where(lane == 8 * b + lax.rem(row + n, 8), line, out)
        return out

    sends = []

    def reduce_begin(r, gram):
        part[r] = gram
        got1[r, slab] = part[r]
        for d in range(1, nslab):
            peer = lax.rem(slab + d, nslab)
            c = remote(part.at[r], got1.at[r, slab], s1_send.at[r, d], s1_recv.at[r, slab], {"slab": peer})
            c.start()
            sends.append(c)

    def reduce_middle(r):
        for d in range(1, nslab):
            peer = lax.rem(slab + d, nslab)
            remote(part.at[r], got1.at[r, peer], s1_send.at[r, d], s1_recv.at[r, peer], {"slab": peer}).wait_recv()
        acc = got1[r, 0]
        for i in range(1, nslab):
            acc = acc + got1[r, i]
        mid[r] = acc
        got2[r, sub] = acc
        for d in range(1, nsub):
            peer = lax.rem(sub + d, nsub)
            c = remote(mid.at[r], got2.at[r, sub], s2_send.at[r, d], s2_recv.at[r, sub], {"sub": peer})
            c.start()
            sends.append(c)

    def reduce_end(r):
        for d in range(1, nsub):
            peer = lax.rem(sub + d, nsub)
            remote(mid.at[r], got2.at[r, peer], s2_send.at[r, d], s2_recv.at[r, peer], {"sub": peer}).wait_recv()
        acc = got2[r, 0]
        for i in range(1, nsub):
            acc = acc + got2[r, i]
        return acc

    up.wait()
    down.wait()
    low = jnp.where(place == 0, 0.0, 1.0).astype(jnp.float32)
    high = jnp.where(place == total - 1, 0.0, 1.0).astype(jnp.float32)
    for k in range(pad):
        a = k * LANES
        ext[:, a : a + LANES] = ext[:, a : a + LANES] * low
        b = (pad + zl + k) * LANES
        ext[:, b : b + LANES] = ext[:, b : b + LANES] * high
    along = lax.rem(lane, nx)

    def fill(e, _):
        def grab(t):
            return ext[:, pl.ds(pl.multiple_of((e + 1 + t) * LANES, LANES), LANES)]

        here, after, before = grab(0), grab(1), grab(-1)
        swap_up = pltpu.roll(here, LANES - nx, 1)
        swap_down = pltpu.roll(here, nx, 1)
        x_up = jnp.where(along == nx - 1, 0.0, pltpu.roll(here, LANES - 1, 1))
        x_down = jnp.where(along == 0, 0.0, pltpu.roll(here, 1, 1))
        swap_up = jnp.where(lane >= LANES - nx, 0.0, swap_up)
        swap_down = jnp.where(lane < nx, 0.0, swap_down)

        def line(value, y):
            return jnp.broadcast_to(value[y : y + 1, :], (8, LANES))

        for y in range(yl_n):
            p = line(here, y)
            others = (
                line(x_up, y),
                line(x_down, y),
                line(here, y + 1) if y + 1 < yl_n else line(swap_up, 0),
                line(here, y - 1) if y > 0 else line(swap_down, yl_n - 1),
                line(after, y),
                line(before, y),
            )
            at = pl.ds(pl.multiple_of((e * yl_n + y) * LANES, LANES), LANES)
            diag = line(here, yl_n + y)
            weights = []
            for q in others:
                both = p * q
                weight = jnp.where(both > 0.0, 2.0 * both / jnp.where(both > 0.0, p + q, 1.0), 0.0)
                weights.append(weight)
                diag = diag + weight
            over = jnp.where(diag > 0.0, 1.0 / jnp.where(diag > 0.0, diag, 1.0), 0.0)
            for k, weight in enumerate(weights):
                coef[k, :, at] = weight * over
            inv[:, at] = over
            diag_own[:, at] = diag
        return 0

    lax.fori_loop(0, span, fill, 0)

    def scale(lo, hi):
        for k in range(lo * yl_n, hi * yl_n):
            at = slice(k * LANES, (k + 1) * LANES)
            first_field[:, at] = basis[0, :, at] * inv[:, at]

    scale(halo, halo + zl)

    first, steps = chebyshev_steps()

    def spot(e, y):
        if isinstance(e, int):
            return pl.ds((e * yl_n + y) * LANES, LANES)
        return pl.ds(pl.multiple_of((e * yl_n + y) * LANES, LANES), LANES)

    def beside(field, e):
        here = [field[:, spot(e, y)] for y in range(yl_n)]
        outs = []
        for y in range(yl_n):
            at = spot(e, y)
            f = here[y]
            y_up = here[y + 1] if y + 1 < yl_n else pltpu.roll(here[0], LANES - nx, 1)
            y_down = here[y - 1] if y > 0 else pltpu.roll(here[yl_n - 1], nx, 1)
            acc = coef[0, :, at] * pltpu.roll(f, LANES - 1, 1)
            acc = acc + coef[1, :, at] * pltpu.roll(f, 1, 1)
            acc = acc + coef[2, :, at] * y_up
            acc = acc + coef[3, :, at] * y_down
            acc = acc + coef[4, :, at] * field[:, spot(e + 1, y)]
            acc = acc + coef[5, :, at] * field[:, spot(e - 1, y)]
            outs.append(acc)
        return here, outs

    def field_of(j):
        return first_field if j == 0 else basis.at[j]

    def advance(j, t, planes):
        fields = (field_of(j), d1, d2, d3)
        source = fields[t]
        for e in planes:
            here, outs = beside(source, e)
            for y in range(yl_n):
                at = spot(e, y)
                if t < DEG - 1:
                    keep, gain = steps[t]
                    if t == 0:
                        r = here[y] - first * (here[y] - outs[y])
                        d = (keep * first) * here[y] + gain * r
                    else:
                        r = rem[:, at] - here[y] + outs[y]
                        d = keep * here[y] + gain * r
                    rem[:, at] = r
                    fields[t + 1][:, at] = d
                    continue
                r = rem[:, at] - here[y] + outs[y]
                value = r * (1.0 / SPREAD) if j == 0 else r * (2.0 / SPREAD) - field_of(j - 1)[:, at]
                if j + 1 < ITERS:
                    basis[j + 1, :, at] = value
                if halo <= e < halo + zl:
                    to = spot(e - halo, y)
                    big[8 * (j + 1) : 8 * (j + 2), to] = value * diag_own[:, at]
                    found[8 * j : 8 * (j + 1), to] = first * fields[0][:, at] + d1[:, at] + d2[:, at] + here[y]

    moves = first_swap
    for j in range(ITERS):
        inset = DEG * (j % REACH)
        if not inset:
            for t in range(DEG):
                advance(j, t, range(halo + t + 1, halo + zl - t - 1))
            reduce_begin(j, products(j))
            if j:
                reduce_middle(j - 1)
            for c in moves:
                c.wait()
            if not j:
                scale(0, halo)
                scale(halo + zl, span)
            for t in range(DEG):
                outer = [*range(t + 1, halo + t + 1), *range(halo + zl - t - 1, span - t - 1)]
                advance(j, t, outer)
        else:
            for t in range(DEG):
                advance(j, t, range(inset + t + 1, span - inset - t - 1))
        if (j + 1) % REACH == 0 and j + 1 < ITERS:
            moves = swap(j + 1, (j + 1) // REACH)
            for c in moves:
                c.start()
        else:
            reduce_begin(j + 1, products(j + 1))
            reduce_middle(j)
    reduce_middle(ITERS)

    rows = 8 * ITERS
    for r in range(ITERS + 1):
        square[8 * r : 8 * r + 8, :] = reduce_end(r)
    turned = square[...].T
    gram = [
        jnp.where(lane < 8 * (r + 1), square[8 * r : 8 * r + 8, :], turned[8 * r : 8 * r + 8, :])
        for r in range(ITERS + 1)
    ]
    up_by = jnp.where(lane < 8, SPREAD, 0.5 * SPREAD)
    down_by = jnp.where(lane < 8, 0.0, 0.5 * SPREAD)
    system = []
    for j in range(ITERS):
        mixed = gram[j] - SPREAD * gram[1] if j == 0 else gram[j] - (0.5 * SPREAD) * (gram[j + 1] + gram[j - 1])
        both = mixed - up_by * pltpu.roll(mixed, LANES - 8, 1) - down_by * pltpu.roll(mixed, 8, 1)
        right = pltpu.roll(mixed, rows, 1)
        system.append(jnp.where(lane < rows, both, jnp.where(lane < rows + 8, right, 0.0)))
    solved = block_jordan(system, row)
    filled = jnp.concatenate([*solved, jnp.zeros((LANES - rows, LANES), jnp.float32)], axis=0)
    mix = filled.T[rows : rows + 8, :]
    used = mix - pltpu.roll(mix * up_by, 8, 1) - pltpu.roll(mix * down_by, LANES - 8, 1)
    leaving = []

    def deliver(f, k, peer):
        return remote(
            out_buf.at[peer, f * yl_n : (f + 1) * yl_n],
            out_got.at[f * yl_n : (f + 1) * yl_n, rows_of(sub), :],
            out_send.at[f, k], out_recv.at[f, sub], {"sub": peer},
        )

    for f in range(2):
        if f == 0:
            mixture = full(((1,), (0,)), mix[:, 0:rows], found[...])
        else:
            mixture = big[0:8, :] - full(((1,), (0,)), used[:, 0 : rows + 8], big[...])
        for k in range(zl * yl_n):
            out_ref[f, k * 8 : k * 8 + 8, :] = mixture[:, k * LANES : (k + 1) * LANES]
        raw_ref[...] = full(((1,), (1,)), out_ref[f], pick_ref[...])
        for y in range(yl_n):
            items = [raw_ref[pl.ds(y * 8 + i, zl, stride=yl_n * 8), :] for i in range(nsub)]
            for i, value in enumerate(butterfly(items)):
                out_buf[i, f * yl_n + y] = value
        for d in range(1, nsub):
            c = deliver(f, d, lax.rem(sub + d, nsub))
            c.start()
            leaving.append(c)
        out_got[f * yl_n : (f + 1) * yl_n, rows_of(sub), :] = out_buf[sub, f * yl_n : (f + 1) * yl_n]
    for f, ref in enumerate((out0_ref, out1_ref)):
        for d in range(1, nsub):
            peer = lax.rem(sub + d, nsub)
            remote(
                out_buf.at[peer, f * yl_n : (f + 1) * yl_n],
                out_got.at[f * yl_n : (f + 1) * yl_n, rows_of(peer), :],
                out_send.at[f, d], out_recv.at[f, peer], {"sub": peer},
            ).wait_recv()
        for y in range(yl_n):
            ref[pl.ds(y, LANES, stride=yl_n), :] = out_got[f * yl_n + y].T
    for c in arrivals + leaving + sends:
        c.wait_send()


def fast_body(rhs, perm, accum, counts):
    nsub, nslab = lax.axis_size("sub"), lax.axis_size("slab")
    s, depth, cy, zs = rhs.shape
    nx = depth * nsub
    pack = LANES // nx
    yl = cy // pack
    zl = zs // nsub
    halo = DEG * REACH
    span = zl + 2 * halo
    pad = halo + 1

    wide = span * yl * LANES
    own = zl * yl * LANES
    f32 = jnp.float32
    rounds = ITERS + 1
    dma = pltpu.SemaphoreType.DMA
    out = pl.pallas_call(
        functools.partial(kernel, (nsub, nslab, zl, yl, pack, nx)),
        out_shape=[jax.ShapeDtypeStruct((s * depth * cy, zs), f32)] * 2,
        in_specs=[pl.BlockSpec(memory_space=pltpu.HBM)] * 4,
        out_specs=[pl.BlockSpec(memory_space=pltpu.VMEM)] * 2,
        scratch_shapes=[
            pltpu.VMEM((s * depth * cy, zs), f32),
            pltpu.VMEM((depth * cy, zs), f32),
            pltpu.VMEM((depth * cy, zs), f32),
            pltpu.SMEM((nsub,), jnp.int32),
            dma((4,)),
            pltpu.VMEM((LANES, LANES), f32),
            pltpu.VMEM((zl * yl * s, LANES), f32),
            pltpu.VMEM((2, zl * yl * s, LANES), f32),
            pltpu.VMEM((yl + 1, zs, LANES), f32),
            pltpu.VMEM((nsub, yl + 1, zl, LANES), f32),
            pltpu.VMEM((nsub, 2 * yl, zl, LANES), f32),
            pltpu.VMEM((2 * yl, zs, LANES), f32),
            pltpu.VMEM((8, (zl + 2 * pad) * LANES), f32),
            pltpu.VMEM((6, 8, wide), f32),
            pltpu.VMEM((8, wide), f32),
            pltpu.VMEM((8, wide), f32),
            pltpu.VMEM((8, wide), f32),
            pltpu.VMEM((ITERS, 8, wide), f32),
            pltpu.VMEM((8 * rounds, own), f32),
            pltpu.VMEM((8 * ITERS, own), f32),
            pltpu.VMEM((8, wide), f32),
            pltpu.VMEM((8, wide), f32),
            pltpu.VMEM((8, wide), f32),
            pltpu.VMEM((8, wide), f32),
            pltpu.VMEM((rounds, 8, LANES), f32),
            pltpu.VMEM((rounds, nslab, 8, LANES), f32),
            pltpu.VMEM((rounds, 8, LANES), f32),
            pltpu.VMEM((rounds, nsub, 8, LANES), f32),
            pltpu.VMEM((LANES, LANES), f32),
            dma((2, nsub)),
            dma((2, nsub)),
            dma((2, nsub)),
            dma((2, nsub)),
            dma((2,)),
            dma((2,)),
            dma((ITERS // REACH, 2)),
            dma((ITERS // REACH, 2)),
            dma((rounds, nslab)),
            dma((rounds, nslab)),
            dma((rounds, nsub)),
            dma((rounds, nsub)),
        ],
        compiler_params=pltpu.CompilerParams(
            collective_id=0, has_side_effects=True, vmem_limit_bytes=60*1024*1024
        ),
    )(rhs.reshape(-1, zs), perm.reshape(-1, zs), accum.reshape(-1, zs), counts)
    return out[0].reshape(rhs.shape), out[1].reshape(rhs.shape)


def choose(rhs, perm, accum, counts):
    nsub = lax.axis_size("sub")
    s, depth, cy, zs = rhs.shape
    nx = depth * nsub
    fits = s == S == nsub == 8 and zs == LANES and zs // nsub % 8 == 0 and LANES % nx == 0 and zs % nsub == 0 and zs // nsub > DEG * REACH
    fits = fits and cy % max(LANES // nx, 1) == 0 and cy // max(LANES // nx, 1) == 4
    if fits:
        return fast_body(rhs, perm, accum, counts)
    return body(rhs, perm, accum, counts)


def solution(mesh):
    placed = (P(None, "sub", None, "slab"), P("sub", None, "slab"), P("sub", None, "slab"), P())
    return jax.shard_map(
        choose,
        mesh=mesh,
        in_specs=placed,
        out_specs=(P(None, "sub", None, "slab"), P(None, "sub", None, "slab")),
        check_vma=False,
    )
```

```python
import functools

import jax
import jax.numpy as jnp
from jax import lax
from jax.experimental import pallas as pl
from jax.experimental.pallas import tpu as pltpu
from jax.sharding import PartitionSpec as P

S = 8
ITERS = 4
DEG = 4


cheb_low = 0.05
cheb_high = 2.0


def with_halo(cells, sides, width):
    for axis, dim in sides:
        count = lax.axis_size(axis)
        ends = count - 1
        head = lax.slice_in_dim(cells, 0, width, axis=dim)
        tail = lax.slice_in_dim(cells, cells.shape[dim] - width, cells.shape[dim], axis=dim)
        cells = jnp.concatenate(
            [
                lax.ppermute(tail, axis, [(i, (i + 1) % count) for i in range(ends)]),
                cells,
                lax.ppermute(head, axis, [((i + 1) % count, i) for i in range(ends)]),
            ],
            axis=dim,
        )
    return cells


def neighbours(field, live, plane):
    first = field[:, 0]
    last = lax.dynamic_index_in_dim(field, live - 1, 1, keepdims=False)
    edges = with_halo(jnp.stack([first, last], axis=1), (("sub", 1),), 1)
    before = edges[:, 0:1]
    after = edges[:, 3:4]
    zero_plane = jnp.zeros_like(field[:, :1])
    up_inside = jnp.concatenate([field[:, 1:], zero_plane], axis=1)
    down_inside = jnp.concatenate([zero_plane, field[:, :-1]], axis=1)
    x_next = jnp.where(plane == live - 1, after, up_inside)
    x_prev = jnp.where(plane == 0, before, down_inside)
    zero_row = jnp.zeros_like(field[:, :, :1])
    y_next = jnp.concatenate([field[:, :, 1:], zero_row], axis=2)
    y_prev = jnp.concatenate([zero_row, field[:, :, :-1]], axis=2)
    padded = with_halo(field, (("slab", 3),), 1)
    z_next = padded[..., 2:]
    z_prev = padded[..., :-2]
    return (x_next, x_prev, y_next, y_prev, z_next, z_prev)


def product(left, right):
    return lax.dot_general(
        left.reshape(left.shape[0], -1),
        right.reshape(right.shape[0], -1),
        (((1,), (1,)), ((), ())),
        precision=lax.Precision.HIGHEST,
    )


def combine(coef, block):
    flat = jnp.dot(coef, block.reshape(block.shape[0], -1), precision=lax.Precision.HIGHEST)
    return flat.reshape(block.shape)


def lower_solve(factor, block):
    flat = jax.scipy.linalg.solve_triangular(factor, block.reshape(block.shape[0], -1), lower=True)
    return flat.reshape(block.shape)


def precondition(vector, operate, inv_diag):
    theta = 0.5 * (cheb_high + cheb_low)
    delta = 0.5 * (cheb_high - cheb_low)
    sigma = theta / delta
    remain = vector
    update = inv_diag * remain * (1.0 / theta)
    result = update
    rho = 1.0 / sigma
    for step in range(DEG - 1):
        remain = remain - operate(update)
        rho_next = 1.0 / (2.0 * sigma - rho)
        update = rho_next * rho * update + 2.0 * rho_next / delta * (inv_diag * remain)
        result = result + update
        rho = rho_next
    return result


def small_solve(coefs, lowers, lead):
    hess = jnp.zeros((ITERS * S, (ITERS + 1) * S), jnp.float32)
    for j in range(ITERS):
        for i in range(j + 1):
            hess = hess.at[j * S : (j + 1) * S, i * S : (i + 1) * S].set(coefs[j][i])
        hess = hess.at[j * S : (j + 1) * S, (j + 1) * S : (j + 2) * S].set(lowers[j])
    target = jnp.zeros((S, (ITERS + 1) * S), jnp.float32).at[:, :S].set(lead)
    normal = jnp.dot(hess, hess.T, precision=lax.Precision.HIGHEST)
    right = jnp.dot(hess, target.T, precision=lax.Precision.HIGHEST)
    factor = jnp.linalg.cholesky(normal)
    mix = jax.scipy.linalg.cho_solve((factor, True), right).T
    return (mix, hess, target)


def body(rhs, perm, accum, counts):
    live = counts[lax.axis_index("sub")]
    depth = rhs.shape[1]
    plane = lax.broadcasted_iota(jnp.int32, (1, depth, 1, 1), 1)
    mask = (plane < live).astype(jnp.float32)
    field_perm = perm[None]
    near = neighbours(field_perm, live, plane)
    conduct = []
    diag = accum[None]
    for other in near:
        weight = 2.0 * field_perm * other / (field_perm + other)
        conduct.append(weight)
        diag = diag + weight
    inv_diag = mask / diag

    def operate(field):
        beside = neighbours(field, live, plane)
        total = diag * field
        for weight, other in zip(conduct, beside):
            total = total - weight * other
        return mask * total

    start = rhs * mask
    lead = jnp.linalg.cholesky(lax.psum(product(start, start), ("sub", "slab")))
    basis = [lower_solve(lead, start)]
    coefs = []
    lowers = []
    for step in range(ITERS):
        direction = precondition(basis[step], operate, inv_diag)
        work = operate(direction)
        stacked, whole = lax.psum(
            (jnp.stack([product(work, basis[i]) for i in range(step + 1)]), product(work, work)),
            ("sub", "slab"),
        )
        found = [stacked[i] for i in range(step + 1)]
        block = whole
        for i in range(step + 1):
            work = work - combine(found[i], basis[i])
            block = block - jnp.dot(found[i], found[i].T, precision=lax.Precision.HIGHEST)
        lower = jnp.linalg.cholesky(block)
        basis.append(lower_solve(lower, work))
        coefs.append(found)
        lowers.append(lower)
    mix, hess, target = small_solve(coefs, lowers, lead)
    combo = combine(mix[:, :S], basis[0])
    for j in range(1, ITERS):
        combo = combo + combine(mix[:, j * S : (j + 1) * S], basis[j])
    solution = precondition(combo, operate, inv_diag)
    residual = start - operate(solution)
    return (solution, residual)

LANES = 128


def full(dims, left, right):
    return lax.dot_general(
        left,
        right,
        (dims, ((), ())),
        precision=lax.Precision.HIGHEST,
        preferred_element_type=jnp.float32,
    )


def chebyshev_steps():
    theta = 0.5 * (cheb_high + cheb_low)
    delta = 0.5 * (cheb_high - cheb_low)
    sigma = theta / delta
    rho = 1.0 / sigma
    steps = []
    for _ in range(DEG - 1):
        rho_next = 1.0 / (2.0 * sigma - rho)
        steps.append((rho_next * rho, 2.0 * rho_next / delta))
        rho = rho_next
    return 1.0 / theta, steps


def spread_rows(value, k):
    return jnp.broadcast_to(value[k : k + 1, :], value.shape)


def spread_lane(value, k):
    return jnp.broadcast_to(value[:, k : k + 1], value.shape)


def times(columns, block):
    total = columns[0] * spread_rows(block, 0)
    for c in range(1, 8):
        total = total + columns[c] * spread_rows(block, c)
    return total


def invert(cols, row):
    cols = list(cols)
    for k in range(8):
        over = 1.0 / spread_rows(cols[k], k)
        pivot = cols[k]
        for c in range(8):
            if c == k:
                cols[c] = jnp.where(row == k, over, -pivot * over)
            else:
                scaled = spread_rows(cols[c], k) * over
                cols[c] = jnp.where(row == k, scaled, cols[c] - pivot * scaled)
    return cols


def block_jordan(blocks, row):
    blocks = list(blocks)
    for k in range(len(blocks)):
        cols = [[spread_lane(b, 8 * k + c) for c in range(8)] for b in blocks]
        solved = times(invert(cols[k], row), blocks[k])
        for i in range(len(blocks)):
            blocks[i] = solved if i == k else blocks[i] - times(cols[i], solved)
    return blocks


SPREAD = 0.52
REACH = 2


def kernel(
    dims,
    rhs_hbm, perm_hbm, accum_hbm, counts_hbm, out0_ref, out1_ref,
    rhs_ref, perm_ref, accum_ref, counts_ref, load_sem,
    pick_ref, ends_ref, raw_ref, out_ref, flux_ref, in_buf, in_got, out_buf, out_got, rim_buf, rim_got,
    wall, edge_ref,
    ext, coef, inv, diag_own, first_field, basis, big, found, d1, d2, d3, rem,
    part, got1, mid, got2, square,
    in_send, in_recv, out_send, out_recv, xs_send, xs_recv, halo_send, halo_recv, s1_send, s1_recv, s2_send, s2_recv,
):
    nsub, nslab, zl, yl_n, pack, nx = dims
    halo = DEG * REACH
    pad = halo + 1
    span = zl + 2 * halo
    per = yl_n + 1
    sub = lax.axis_index("sub")
    slab = lax.axis_index("slab")

    total = nsub * nslab
    layer, core = slab // 2, lax.rem(slab, 2)
    at = sub // 2 + lax.rem(sub, 2) * (nsub - 1 - 2 * (sub // 2))
    at = at + lax.rem(layer, 2) * (nsub - 1 - 2 * at)
    place = 2 * (layer * nsub + at) + core
    home, mine = place // nsub, lax.rem(place, nsub)
    nxt = lax.rem(place + 1, total)
    prv = lax.rem(place + total - 1, total)

    def dev(g):
        chip = g // 2
        layer = chip // nsub
        at = lax.rem(chip, nsub)
        at = at + lax.rem(layer, 2) * (nsub - 1 - 2 * at)
        across = at // (nsub // 2)
        return {"sub": 2 * (at + across * (nsub - 1 - 2 * at)) + across, "slab": 2 * layer + lax.rem(g, 2)}

    loads = [
        pltpu.make_async_copy(src, dst, load_sem.at[k])
        for k, (src, dst) in enumerate(
            ((perm_hbm, perm_ref), (accum_hbm, accum_ref), (rhs_hbm, rhs_ref), (counts_hbm, counts_ref))
        )
    ]
    for c in loads:
        c.start()

    barrier = pltpu.get_barrier_semaphore()
    peers = [{"slab": lax.rem(slab + d, nslab)} for d in range(1, nslab)]
    for d in range(1, nsub):
        peers += [{"sub": lax.rem(sub + d, nsub)}, {"sub": lax.rem(sub + d, nsub), "slab": 2 * layer + 1 - core}]
    for device in peers:
        pl.semaphore_signal(barrier, inc=1, device_id=device, device_id_type=pl.DeviceIdType.MESH)

    def remote(src, dst, send, recv, device):
        return pltpu.make_async_remote_copy(
            src_ref=src, dst_ref=dst, send_sem=send, recv_sem=recv,
            device_id=device, device_id_type=pl.DeviceIdType.MESH,
        )

    group = pack * (LANES // (pack * nsub))
    square[...] = jnp.zeros_like(square)
    for c in loads:
        c.wait()
    pieces = [ref[pl.ds(y, group, stride=yl_n), :] for ref in (perm_ref, accum_ref) for y in range(yl_n)]
    in_buf[yl_n] = jnp.concatenate(pieces, axis=0).T
    for y in range(yl_n):
        in_buf[y] = rhs_ref[pl.ds(y, LANES, stride=yl_n), :].T

    pl.semaphore_wait(barrier, len(peers))

    def rows_of(i):
        return pl.ds(pl.multiple_of(i * zl, 8), zl)

    halves = ((yl_n, 1), (0, yl_n))
    arrivals = []
    for k, (t, n) in enumerate(halves):
        for d in range(nsub):
            q = lax.rem(mine + d, nsub)
            goal = slab * nsub + q
            c = remote(
                in_buf.at[t : t + n, rows_of(q), :], in_got.at[sub, t : t + n],
                in_send.at[k, d], in_recv.at[k, sub], dev(goal),
            )
            pl.when(goal != place)(c.start)
            arrivals.append((goal != place, c))

    @pl.when(home == slab)
    def _():
        in_got[sub] = in_buf[:, rows_of(mine), :]

    def arrived(k):
        t, n = halves[k]
        for i in range(nsub):
            c = remote(
                in_buf.at[t : t + n, 0:zl, :], in_got.at[i, t : t + n],
                in_send.at[k, i], in_recv.at[k, i], {"sub": i, "slab": home},
            )
            pl.when((home != slab) | (sub != i))(c.wait_recv)

    wide_row = lax.broadcasted_iota(jnp.int32, (LANES, LANES), 0)
    wide_lane = lax.broadcasted_iota(jnp.int32, (LANES, LANES), 1)
    rank = lax.rem(wide_row, group) // pack
    owner = wide_row // group
    base_of = jnp.zeros_like(wide_row)
    live_of = jnp.zeros_like(wide_row)
    before = jnp.int32(0)
    for i in range(nsub):
        live = counts_ref[i]
        base_of = jnp.where(owner == i, before, base_of)
        live_of = jnp.where(owner == i, live, live_of)
        before = before + live
    goal = base_of + rank + lax.rem(wide_row, pack) * nx
    pick_ref[...] = jnp.where((rank < live_of) & (goal == wide_lane), 1.0, 0.0).astype(jnp.float32)

    owner = wide_lane // group
    target = jnp.zeros_like(wide_row)
    before = jnp.int32(0)
    for i in range(nsub):
        face = before - 1 + lax.rem(wide_lane // 8, 2) * counts_ref[i]
        target = jnp.where(owner == i, face, target)
        before = before + counts_ref[i]
    at_face = (lax.rem(wide_row, nx) == target) & (wide_row // nx == lax.rem(wide_lane // yl_n, 2))
    for y in range(yl_n):
        ends_ref[y] = jnp.where(at_face & (lax.rem(wide_lane, yl_n) == y), 1.0, 0.0).astype(jnp.float32)

    live_here = counts_ref[sub]
    depth = perm_ref.shape[0] // 8

    def plane(p):
        return slice(8 * p, 8 * p + 8)

    tall = lax.broadcasted_iota(jnp.int32, (8, LANES), 0)
    long = lax.broadcasted_iota(jnp.int32, (8, LANES), 1)
    for p in range(depth):
        mine_perm = perm_ref[plane(p), :]
        alive = jnp.where(p < live_here, 2.0, 0.0).astype(jnp.float32)
        if p + 1 < depth:
            other = perm_ref[plane(p + 1), :]
            joined = jnp.where(p + 1 < live_here, 2.0, 0.0).astype(jnp.float32)
            wall[0, plane(p), :] = joined * mine_perm * other / (mine_perm + other)
        other = pltpu.roll(mine_perm, 7, 0)
        wall[1, plane(p), :] = jnp.where(tall < 7, alive * mine_perm * other / (mine_perm + other), 0.0)
        other = pltpu.roll(mine_perm, LANES - 1, 1)
        wall[2, plane(p), :] = jnp.where(long < LANES - 1, alive * mine_perm * other / (mine_perm + other), 0.0)

    strip = lax.broadcasted_iota(jnp.int32, (zl, LANES), 1) // group

    def butterfly(items):
        d = len(items) // 2
        while d:
            fresh = list(items)
            for a in range(len(items)):
                if a & d:
                    continue
                first_half = (strip[0 : items[a].shape[0], :] & d) == 0
                fresh[a] = jnp.where(first_half, items[a], pltpu.roll(items[a + d], group * d, 1))
                fresh[a + d] = jnp.where(first_half, pltpu.roll(items[a], LANES - group * d, 1), items[a + d])
            items = fresh
            d //= 2
        return items

    lane = lax.broadcasted_iota(jnp.int32, (8, LANES), 1)
    row = lax.broadcasted_iota(jnp.int32, (8, LANES), 0)
    tile = yl_n * LANES
    side = halo * tile
    own_lo, own_hi = side, side + zl * tile

    arrived(0)
    for i, value in enumerate(butterfly([in_got[i, yl_n] for i in range(nsub)])):
        raw_ref[pl.ds(i, zl, stride=8), :] = value
    packed = full(((1,), (0,)), raw_ref[0 : zl * 8, :], pick_ref[...])
    for k in range(zl):
        at = (pad + k) * LANES
        ext[:, at : at + LANES] = packed[k * 8 : k * 8 + 8, :]
    edge = pad * LANES
    whole = zl * LANES
    up = remote(ext.at[:, whole : whole + edge], ext.at[:, 0:edge], xs_send.at[0], xs_recv.at[0], dev(nxt))
    down = remote(ext.at[:, edge : 2 * edge], ext.at[:, edge + whole : 2 * edge + whole], xs_send.at[1], xs_recv.at[1], dev(prv))
    up.start()
    down.start()

    arrived(1)
    for t in range(yl_n):
        for i, value in enumerate(butterfly([in_got[i, t] for i in range(nsub)])):
            raw_ref[pl.ds(t * 8 + i, zl, stride=yl_n * 8), :] = value
    packed = full(((1,), (0,)), raw_ref[...], pick_ref[...])
    for k in range(zl * yl_n):
        basis[0, :, own_lo + k * LANES : own_lo + (k + 1) * LANES] = packed[k * 8 : k * 8 + 8, :]
        big[0:8, k * LANES : (k + 1) * LANES] = packed[k * 8 : k * 8 + 8, :]

    def swap(n, m):
        return [
            remote(
                basis.at[n, :, own_hi - side : own_hi], basis.at[n, :, 0:side],
                halo_send.at[m, 0], halo_recv.at[m, 0], dev(nxt),
            ),
            remote(
                basis.at[n, :, own_lo : own_lo + side], basis.at[n, :, own_hi : own_hi + side],
                halo_send.at[m, 1], halo_recv.at[m, 1], dev(prv),
            ),
        ]

    first_swap = swap(0, 0)
    for c in first_swap:
        c.start()

    def products(j):
        blocks = j + 1

        def add(k, accs):
            accs = list(accs)
            for h in range(2):
                at = pl.ds(pl.multiple_of((2 * k + h) * LANES, LANES), LANES)
                w = big[8 * j : 8 * j + 8, at]
                turned = [w] + [pltpu.roll(w, n, 0) for n in range(1, 8)]
                for b in range(blocks):
                    v = w if b == j else big[8 * b : 8 * b + 8, at]
                    for n in range(8):
                        accs[8 * b + n] = accs[8 * b + n] + v * turned[n]
            return tuple(accs)

        zero = jnp.zeros((8, LANES), jnp.float32)
        accs = lax.fori_loop(0, zl * yl_n // 2, add, (zero,) * (8 * blocks))
        out = zero
        for b in range(blocks):
            for n in range(8):
                acc = accs[8 * b + n]
                acc = pltpu.roll(acc, 8 - n, 0) if n else acc
                line = jnp.sum(acc, axis=1, keepdims=True)
                out = jnp.where(lane == 8 * b + lax.rem(row + n, 8), line, out)
        return out

    sends = []

    def reduce_begin(r, gram):
        part[r] = gram
        got1[r, slab] = part[r]
        for d in range(1, nslab):
            peer = lax.rem(slab + d, nslab)
            c = remote(part.at[r], got1.at[r, slab], s1_send.at[r, d], s1_recv.at[r, slab], {"slab": peer})
            c.start()
            sends.append(c)

    def reduce_middle(r):
        for d in range(1, nslab):
            peer = lax.rem(slab + d, nslab)
            remote(part.at[r], got1.at[r, peer], s1_send.at[r, d], s1_recv.at[r, peer], {"slab": peer}).wait_recv()
        acc = got1[r, 0]
        for i in range(1, nslab):
            acc = acc + got1[r, i]
        mid[r] = acc
        got2[r, sub] = acc
        for d in range(1, nsub):
            peer = lax.rem(sub + d, nsub)
            c = remote(mid.at[r], got2.at[r, sub], s2_send.at[r, d], s2_recv.at[r, sub], {"sub": peer})
            c.start()
            sends.append(c)

    def reduce_end(r):
        for d in range(1, nsub):
            peer = lax.rem(sub + d, nsub)
            remote(mid.at[r], got2.at[r, peer], s2_send.at[r, d], s2_recv.at[r, peer], {"sub": peer}).wait_recv()
        acc = got2[r, 0]
        for i in range(1, nsub):
            acc = acc + got2[r, i]
        return acc

    up.wait()
    down.wait()
    low = jnp.where(place == 0, 0.0, 1.0).astype(jnp.float32)
    high = jnp.where(place == total - 1, 0.0, 1.0).astype(jnp.float32)
    for k in range(pad):
        a = k * LANES
        ext[:, a : a + LANES] = ext[:, a : a + LANES] * low
        b = (pad + zl + k) * LANES
        ext[:, b : b + LANES] = ext[:, b : b + LANES] * high
    along = lax.rem(lane, nx)

    def fill(e, _):
        def grab(t):
            return ext[:, pl.ds(pl.multiple_of((e + 1 + t) * LANES, LANES), LANES)]

        here, after, before = grab(0), grab(1), grab(-1)
        swap_up = pltpu.roll(here, LANES - nx, 1)
        swap_down = pltpu.roll(here, nx, 1)
        x_up = jnp.where(along == nx - 1, 0.0, pltpu.roll(here, LANES - 1, 1))
        x_down = jnp.where(along == 0, 0.0, pltpu.roll(here, 1, 1))
        swap_up = jnp.where(lane >= LANES - nx, 0.0, swap_up)
        swap_down = jnp.where(lane < nx, 0.0, swap_down)

        def line(value, y):
            return jnp.broadcast_to(value[y : y + 1, :], (8, LANES))

        for y in range(yl_n):
            p = line(here, y)
            others = (
                line(x_up, y),
                line(x_down, y),
                line(here, y + 1) if y + 1 < yl_n else line(swap_up, 0),
                line(here, y - 1) if y > 0 else line(swap_down, yl_n - 1),
                line(after, y),
                line(before, y),
            )
            at = pl.ds(pl.multiple_of((e * yl_n + y) * LANES, LANES), LANES)
            diag = line(here, yl_n + y)
            weights = []
            for q in others:
                both = p * q
                weight = jnp.where(both > 0.0, 2.0 * both / jnp.where(both > 0.0, p + q, 1.0), 0.0)
                weights.append(weight)
                diag = diag + weight
            over = jnp.where(diag > 0.0, 1.0 / jnp.where(diag > 0.0, diag, 1.0), 0.0)
            for k, weight in enumerate(weights):
                coef[k, :, at] = weight * over
            inv[:, at] = over
            diag_own[:, at] = diag
        return 0

    lax.fori_loop(0, span, fill, 0)

    def scale(lo, hi):
        for k in range(lo * yl_n, hi * yl_n):
            at = slice(k * LANES, (k + 1) * LANES)
            first_field[:, at] = basis[0, :, at] * inv[:, at]

    scale(halo, halo + zl)

    first, steps = chebyshev_steps()

    def spot(e, y):
        if isinstance(e, int):
            return pl.ds((e * yl_n + y) * LANES, LANES)
        return pl.ds(pl.multiple_of((e * yl_n + y) * LANES, LANES), LANES)

    def beside(field, e):
        here = [field[:, spot(e, y)] for y in range(yl_n)]
        outs = []
        for y in range(yl_n):
            at = spot(e, y)
            f = here[y]
            y_up = here[y + 1] if y + 1 < yl_n else pltpu.roll(here[0], LANES - nx, 1)
            y_down = here[y - 1] if y > 0 else pltpu.roll(here[yl_n - 1], nx, 1)
            acc = coef[0, :, at] * pltpu.roll(f, LANES - 1, 1)
            acc = acc + coef[1, :, at] * pltpu.roll(f, 1, 1)
            acc = acc + coef[2, :, at] * y_up
            acc = acc + coef[3, :, at] * y_down
            acc = acc + coef[4, :, at] * field[:, spot(e + 1, y)]
            acc = acc + coef[5, :, at] * field[:, spot(e - 1, y)]
            outs.append(acc)
        return here, outs

    def field_of(j):
        return first_field if j == 0 else basis.at[j]

    def advance(j, t, planes):
        fields = (field_of(j), d1, d2, d3)
        source = fields[t]
        for e in planes:
            here, outs = beside(source, e)
            for y in range(yl_n):
                at = spot(e, y)
                if t < DEG - 1:
                    keep, gain = steps[t]
                    if t == 0:
                        r = here[y] - first * (here[y] - outs[y])
                        d = (keep * first) * here[y] + gain * r
                    else:
                        r = rem[:, at] - here[y] + outs[y]
                        d = keep * here[y] + gain * r
                    rem[:, at] = r
                    fields[t + 1][:, at] = d
                    continue
                r = rem[:, at] - here[y] + outs[y]
                value = r * (1.0 / SPREAD) if j == 0 else r * (2.0 / SPREAD) - field_of(j - 1)[:, at]
                if j + 1 < ITERS:
                    basis[j + 1, :, at] = value
                if halo <= e < halo + zl:
                    big[8 * (j + 1) : 8 * (j + 2), spot(e - halo, y)] = value * diag_own[:, at]
                if halo - 1 <= e <= halo + zl:
                    found[8 * j : 8 * (j + 1), spot(e - halo + 1, y)] = first * fields[0][:, at] + d1[:, at] + d2[:, at] + here[y]

    moves = first_swap
    for j in range(ITERS):
        inset = DEG * (j % REACH)
        if not inset:
            for t in range(DEG):
                advance(j, t, range(halo + t + 1, halo + zl - t - 1))
            reduce_begin(j, products(j))
            for c in moves:
                c.wait()
            if not j:
                scale(0, halo)
                scale(halo + zl, span)
            for t in range(DEG):
                outer = [*range(t + 1, halo + t + 1), *range(halo + zl - t - 1, span - t - 1)]
                advance(j, t, outer)
        else:
            for t in range(DEG):
                advance(j, t, range(inset + t + 1, span - inset - t - 1))
            for e in (halo - 1, halo + zl):
                for y in range(yl_n):
                    at = spot(e, y)
                    found[8 * j : 8 * (j + 1), spot(e - halo + 1, y)] = (
                        first * field_of(j)[:, at] + d1[:, at] + d2[:, at] + d3[:, at]
                    )
        if (j + 1) % REACH == 0 and j + 1 < ITERS:
            moves = swap(j + 1, (j + 1) // REACH)
            for c in moves:
                c.start()
        else:
            reduce_begin(j + 1, products(j + 1))
        if j == 2:
            for r in range(3):
                reduce_middle(r)
    for r in range(3, ITERS + 1):
        reduce_middle(r)

    rows = 8 * ITERS
    for r in range(ITERS + 1):
        square[8 * r : 8 * r + 8, :] = reduce_end(r)
    turned = square[...].T
    gram = [
        jnp.where(lane < 8 * (r + 1), square[8 * r : 8 * r + 8, :], turned[8 * r : 8 * r + 8, :])
        for r in range(ITERS + 1)
    ]
    up_by = jnp.where(lane < 8, SPREAD, 0.5 * SPREAD)
    down_by = jnp.where(lane < 8, 0.0, 0.5 * SPREAD)
    system = []
    for j in range(ITERS):
        mixed = gram[j] - SPREAD * gram[1] if j == 0 else gram[j] - (0.5 * SPREAD) * (gram[j + 1] + gram[j - 1])
        both = mixed - up_by * pltpu.roll(mixed, LANES - 8, 1) - down_by * pltpu.roll(mixed, 8, 1)
        right = pltpu.roll(mixed, rows, 1)
        system.append(jnp.where(lane < rows, both, jnp.where(lane < rows + 8, right, 0.0)))
    solved = block_jordan(system, row)
    filled = jnp.concatenate([*solved, jnp.zeros((LANES - rows, LANES), jnp.float32)], axis=0)
    mix = filled.T[rows : rows + 8, :]
    leaving = []
    half = zl // 2
    capped = (mine == 0) | (mine == nsub - 1)

    def part_of(f, q, peer):
        if f < 2:
            rows_at = pl.ds(pl.multiple_of(q * zl + f * half, 8), half)
            return out_buf.at[peer, :, f * half : (f + 1) * half, :], out_got.at[:, rows_at, :]
        if f == 2:
            return rim_buf.at[peer, 0:zl], rim_got.at[q, 0:zl]
        return rim_buf.at[peer, zl : zl + 8], rim_got.at[q, zl : zl + 8]

    def send(f):
        for d in range(nsub):
            peer = lax.rem(sub + d, nsub)
            src, dst = part_of(f, mine, peer)
            c = remote(src, dst, out_send.at[f, d], out_recv.at[f, mine], {"sub": peer, "slab": home})
            away = None
            if d == 0:
                away = home != slab
            if f == 3:
                away = capped if away is None else away & capped
            if away is None:
                c.start()
            else:
                pl.when(away)(c.start)
            leaving.append((away, c))

    def landed(f):
        for q in range(nsub) if f < 3 else (0, nsub - 1):
            src, dst = part_of(f, q, 0)
            c = remote(src, dst, out_send.at[f, q], out_recv.at[f, q], dev(slab * nsub + q))
            pl.when(slab * nsub + q != place)(c.wait_recv)

    pieces = []
    for f in range(2):
        lo = (f * (half + 1)) * yl_n * LANES
        hi = lo + (half + 1) * yl_n * LANES
        piece = full(((1,), (0,)), mix[:, 0:rows], found[:, lo:hi])
        pieces.append(piece)
        for e in range(f * half, (f + 1) * half):
            for y in range(yl_n):
                k = (e + 1) * yl_n + y
                at = k * LANES - lo
                k = e * yl_n + y
                if f == 0 or at + LANES <= hi - lo:
                    out_ref[k * 8 : k * 8 + 8, :] = piece[:, at : at + LANES]
        base = f * half * yl_n * 8
        raw_ref[base : base + half * yl_n * 8, :] = full(
            ((1,), (1,)), out_ref[base : base + half * yl_n * 8, :], pick_ref[...]
        )
        for y in range(yl_n):
            items = [raw_ref[pl.ds(base + y * 8 + i, half, stride=yl_n * 8), :] for i in range(nsub)]
            for i, value in enumerate(butterfly(items)):
                out_buf[i, y, f * half : (f + 1) * half, :] = value
        send(f)

    def sol_at(e, y):
        k = (e + 1) * yl_n + y
        f = k // ((half + 1) * yl_n)
        at = (k - f * (half + 1) * yl_n) * LANES
        return pieces[f][:, at : at + LANES]

    @pl.when(home == slab)
    def _():
        out_got[:, rows_of(mine), :] = out_buf[sub]

    for e in range(zl):
        for y in range(yl_n):
            at = spot(halo + e, y)
            k = e * yl_n + y
            value = out_ref[k * 8 : k * 8 + 8, :]
            drop = value - pltpu.roll(value, LANES - 1, 1)
            flux_ref[y, e * 8 : e * 8 + 8, :] = coef[0, :, at] * diag_own[:, at] * drop
    faces = full(((1,), (0,)), flux_ref[0], ends_ref[0])
    for y in range(1, yl_n):
        faces = faces + full(((1,), (0,)), flux_ref[y], ends_ref[y])
    for y in range(yl_n):
        at = spot(halo, y)
        flux_ref[0, y * 8 : y * 8 + 8, :] = coef[5, :, at] * diag_own[:, at] * (sol_at(-1, y) - sol_at(0, y))
        at = spot(halo + zl - 1, y)
        flux_ref[1, y * 8 : y * 8 + 8, :] = coef[4, :, at] * diag_own[:, at] * (sol_at(zl - 1, y) - sol_at(zl, y))
    raw_ref[0 : zl * 8, :] = faces
    for f in range(2):
        raw_ref[zl * 8 + f * yl_n * 8 : zl * 8 + (f + 1) * yl_n * 8, :] = full(
            ((1,), (1,)), flux_ref[f, 0 : yl_n * 8, :], pick_ref[...]
        )
    for i, value in enumerate(butterfly([raw_ref[pl.ds(i, zl, stride=8), :] for i in range(nsub)])):
        rim_buf[i, 0:zl, :] = value
    send(2)
    for i, value in enumerate(butterfly([raw_ref[pl.ds(zl * 8 + i, 8, stride=8), :] for i in range(nsub)])):
        rim_buf[i, zl : zl + 8, :] = value
    send(3)

    @pl.when(home == slab)
    def _():
        rim_got[mine] = rim_buf[sub]

    landed(0)
    landed(1)
    for y in range(yl_n):
        out0_ref[pl.ds(y, LANES, stride=yl_n), :] = out_got[y].T
    landed(2)
    landed(3)
    around = jnp.concatenate([rim_got[q, 0:zl, :] for q in range(nsub)], axis=0).T
    caps = jnp.concatenate(
        [rim_got[0, zl : zl + yl_n, :], rim_got[nsub - 1, zl + yl_n : zl + 8, :], jnp.zeros((LANES - 8, LANES), jnp.float32)],
        axis=0,
    ).T
    for y in range(yl_n):
        lower = jnp.broadcast_to(caps[:, y : y + 1], (LANES, LANES))
        upper = jnp.broadcast_to(caps[:, yl_n + y : yl_n + y + 1], (LANES, LANES))
        edge_ref[pl.ds(y, LANES, stride=yl_n), :] = jnp.where(
            wide_lane == 0, lower, jnp.where(wide_lane == LANES - 1, -upper, 0.0)
        )
    for i in range(8):
        def rows_at(p):
            return slice((i * depth + p) * 8, (i * depth + p + 1) * 8)

        carried = around[16 * i : 16 * i + 8, :]
        beyond = around[16 * i + 8 : 16 * i + 16, :]
        value = out0_ref[rows_at(0), :]
        for p in range(depth):
            alive = jnp.where(p < live_here, 1.0, 0.0).astype(jnp.float32)
            final = jnp.where(p + 1 == live_here, 1.0, 0.0).astype(jnp.float32)
            rest = alive * rhs_ref[rows_at(p), :] + edge_ref[rows_at(p), :] - accum_ref[plane(p), :] * value
            rest = rest + carried - final * beyond
            fy = wall[1, plane(p), :] * (value - pltpu.roll(value, 7, 0))
            fz = wall[2, plane(p), :] * (value - pltpu.roll(value, LANES - 1, 1))
            rest = rest - (fy - pltpu.roll(fy, 1, 0)) - (fz - pltpu.roll(fz, 1, 1))
            if p + 1 < depth:
                ahead = out0_ref[rows_at(p + 1), :]
                carried = wall[0, plane(p), :] * (value - ahead)
                rest = rest - carried
                value = ahead
            out1_ref[rows_at(p), :] = rest
    for away, c in arrivals + leaving:
        if away is None:
            c.wait_send()
        else:
            pl.when(away)(c.wait_send)
    for c in sends:
        c.wait_send()


def fast_body(rhs, perm, accum, counts):
    nsub, nslab = lax.axis_size("sub"), lax.axis_size("slab")
    s, depth, cy, zs = rhs.shape
    nx = depth * nsub
    pack = LANES // nx
    yl = cy // pack
    zl = zs // nsub
    halo = DEG * REACH
    span = zl + 2 * halo
    pad = halo + 1

    wide = span * yl * LANES
    own = zl * yl * LANES
    f32 = jnp.float32
    rounds = ITERS + 1
    dma = pltpu.SemaphoreType.DMA
    out = pl.pallas_call(
        functools.partial(kernel, (nsub, nslab, zl, yl, pack, nx)),
        out_shape=[jax.ShapeDtypeStruct((s * depth * cy, zs), f32)] * 2,
        in_specs=[pl.BlockSpec(memory_space=pltpu.HBM)] * 4,
        out_specs=[pl.BlockSpec(memory_space=pltpu.VMEM)] * 2,
        scratch_shapes=[
            pltpu.VMEM((s * depth * cy, zs), f32),
            pltpu.VMEM((depth * cy, zs), f32),
            pltpu.VMEM((depth * cy, zs), f32),
            pltpu.SMEM((nsub,), jnp.int32),
            dma((4,)),
            pltpu.VMEM((LANES, LANES), f32),
            pltpu.VMEM((yl, LANES, LANES), f32),
            pltpu.VMEM((zl * yl * s, LANES), f32),
            pltpu.VMEM((zl * yl * s, LANES), f32),
            pltpu.VMEM((yl, zl * s, LANES), f32),
            pltpu.VMEM((yl + 1, zs, LANES), f32),
            pltpu.VMEM((nsub, yl + 1, zl, LANES), f32),
            pltpu.VMEM((nsub, yl, zl, LANES), f32),
            pltpu.VMEM((yl, zs, LANES), f32),
            pltpu.VMEM((nsub, zl + 8, LANES), f32),
            pltpu.VMEM((nsub, zl + 8, LANES), f32),
            pltpu.VMEM((3, depth * cy, zs), f32),
            pltpu.VMEM((s * depth * cy, zs), f32),
            pltpu.VMEM((8, (zl + 2 * pad) * LANES), f32),
            pltpu.VMEM((6, 8, wide), f32),
            pltpu.VMEM((8, wide), f32),
            pltpu.VMEM((8, wide), f32),
            pltpu.VMEM((8, wide), f32),
            pltpu.VMEM((ITERS, 8, wide), f32),
            pltpu.VMEM((8 * rounds, own), f32),
            pltpu.VMEM((8 * ITERS, own + 2 * yl * LANES), f32),
            pltpu.VMEM((8, wide), f32),
            pltpu.VMEM((8, wide), f32),
            pltpu.VMEM((8, wide), f32),
            pltpu.VMEM((8, wide), f32),
            pltpu.VMEM((rounds, 8, LANES), f32),
            pltpu.VMEM((rounds, nslab, 8, LANES), f32),
            pltpu.VMEM((rounds, 8, LANES), f32),
            pltpu.VMEM((rounds, nsub, 8, LANES), f32),
            pltpu.VMEM((LANES, LANES), f32),
            dma((2, nsub)),
            dma((2, nsub)),
            dma((4, nsub)),
            dma((4, nsub)),
            dma((2,)),
            dma((2,)),
            dma((ITERS // REACH, 2)),
            dma((ITERS // REACH, 2)),
            dma((rounds, nslab)),
            dma((rounds, nslab)),
            dma((rounds, nsub)),
            dma((rounds, nsub)),
        ],
        compiler_params=pltpu.CompilerParams(
            collective_id=0, has_side_effects=True, vmem_limit_bytes=60*1024*1024
        ),
    )(rhs.reshape(-1, zs), perm.reshape(-1, zs), accum.reshape(-1, zs), counts)
    return out[0].reshape(rhs.shape), out[1].reshape(rhs.shape)


def choose(rhs, perm, accum, counts):
    nsub = lax.axis_size("sub")
    s, depth, cy, zs = rhs.shape
    nx = depth * nsub
    fits = s == S == nsub == 8 and zs == LANES and depth == cy == 8 and zs // nsub % 8 == 0 and LANES % nx == 0 and zs % nsub == 0 and lax.axis_size("slab") % 2 == 0 and zs // nsub > DEG * REACH
    fits = fits and cy % max(LANES // nx, 1) == 0 and cy // max(LANES // nx, 1) == 4
    if fits:
        return fast_body(rhs, perm, accum, counts)
    return body(rhs, perm, accum, counts)


def solution(mesh):
    placed = (P(None, "sub", None, "slab"), P("sub", None, "slab"), P("sub", None, "slab"), P())
    return jax.shard_map(
        choose,
        mesh=mesh,
        in_specs=placed,
        out_specs=(P(None, "sub", None, "slab"), P(None, "sub", None, "slab")),
        check_vma=False,
    )
```

```python
import functools

import jax
import jax.numpy as jnp
from jax import lax
from jax.experimental import pallas as pl
from jax.experimental.pallas import tpu as pltpu
from jax.sharding import PartitionSpec as P

S = 8
ITERS = 4
DEG = 4


cheb_low = 0.05
cheb_high = 2.0


def with_halo(cells, sides, width):
    for axis, dim in sides:
        count = lax.axis_size(axis)
        ends = count - 1
        head = lax.slice_in_dim(cells, 0, width, axis=dim)
        tail = lax.slice_in_dim(cells, cells.shape[dim] - width, cells.shape[dim], axis=dim)
        cells = jnp.concatenate(
            [
                lax.ppermute(tail, axis, [(i, (i + 1) % count) for i in range(ends)]),
                cells,
                lax.ppermute(head, axis, [((i + 1) % count, i) for i in range(ends)]),
            ],
            axis=dim,
        )
    return cells


def neighbours(field, live, plane):
    first = field[:, 0]
    last = lax.dynamic_index_in_dim(field, live - 1, 1, keepdims=False)
    edges = with_halo(jnp.stack([first, last], axis=1), (("sub", 1),), 1)
    before = edges[:, 0:1]
    after = edges[:, 3:4]
    zero_plane = jnp.zeros_like(field[:, :1])
    up_inside = jnp.concatenate([field[:, 1:], zero_plane], axis=1)
    down_inside = jnp.concatenate([zero_plane, field[:, :-1]], axis=1)
    x_next = jnp.where(plane == live - 1, after, up_inside)
    x_prev = jnp.where(plane == 0, before, down_inside)
    zero_row = jnp.zeros_like(field[:, :, :1])
    y_next = jnp.concatenate([field[:, :, 1:], zero_row], axis=2)
    y_prev = jnp.concatenate([zero_row, field[:, :, :-1]], axis=2)
    padded = with_halo(field, (("slab", 3),), 1)
    z_next = padded[..., 2:]
    z_prev = padded[..., :-2]
    return (x_next, x_prev, y_next, y_prev, z_next, z_prev)


def product(left, right):
    return lax.dot_general(
        left.reshape(left.shape[0], -1),
        right.reshape(right.shape[0], -1),
        (((1,), (1,)), ((), ())),
        precision=lax.Precision.HIGHEST,
    )


def combine(coef, block):
    flat = jnp.dot(coef, block.reshape(block.shape[0], -1), precision=lax.Precision.HIGHEST)
    return flat.reshape(block.shape)


def lower_solve(factor, block):
    flat = jax.scipy.linalg.solve_triangular(factor, block.reshape(block.shape[0], -1), lower=True)
    return flat.reshape(block.shape)


def precondition(vector, operate, inv_diag):
    theta = 0.5 * (cheb_high + cheb_low)
    delta = 0.5 * (cheb_high - cheb_low)
    sigma = theta / delta
    remain = vector
    update = inv_diag * remain * (1.0 / theta)
    result = update
    rho = 1.0 / sigma
    for step in range(DEG - 1):
        remain = remain - operate(update)
        rho_next = 1.0 / (2.0 * sigma - rho)
        update = rho_next * rho * update + 2.0 * rho_next / delta * (inv_diag * remain)
        result = result + update
        rho = rho_next
    return result


def small_solve(coefs, lowers, lead):
    hess = jnp.zeros((ITERS * S, (ITERS + 1) * S), jnp.float32)
    for j in range(ITERS):
        for i in range(j + 1):
            hess = hess.at[j * S : (j + 1) * S, i * S : (i + 1) * S].set(coefs[j][i])
        hess = hess.at[j * S : (j + 1) * S, (j + 1) * S : (j + 2) * S].set(lowers[j])
    target = jnp.zeros((S, (ITERS + 1) * S), jnp.float32).at[:, :S].set(lead)
    normal = jnp.dot(hess, hess.T, precision=lax.Precision.HIGHEST)
    right = jnp.dot(hess, target.T, precision=lax.Precision.HIGHEST)
    factor = jnp.linalg.cholesky(normal)
    mix = jax.scipy.linalg.cho_solve((factor, True), right).T
    return (mix, hess, target)


def body(rhs, perm, accum, counts):
    live = counts[lax.axis_index("sub")]
    depth = rhs.shape[1]
    plane = lax.broadcasted_iota(jnp.int32, (1, depth, 1, 1), 1)
    mask = (plane < live).astype(jnp.float32)
    field_perm = perm[None]
    near = neighbours(field_perm, live, plane)
    conduct = []
    diag = accum[None]
    for other in near:
        weight = 2.0 * field_perm * other / (field_perm + other)
        conduct.append(weight)
        diag = diag + weight
    inv_diag = mask / diag

    def operate(field):
        beside = neighbours(field, live, plane)
        total = diag * field
        for weight, other in zip(conduct, beside):
            total = total - weight * other
        return mask * total

    start = rhs * mask
    lead = jnp.linalg.cholesky(lax.psum(product(start, start), ("sub", "slab")))
    basis = [lower_solve(lead, start)]
    coefs = []
    lowers = []
    for step in range(ITERS):
        direction = precondition(basis[step], operate, inv_diag)
        work = operate(direction)
        stacked, whole = lax.psum(
            (jnp.stack([product(work, basis[i]) for i in range(step + 1)]), product(work, work)),
            ("sub", "slab"),
        )
        found = [stacked[i] for i in range(step + 1)]
        block = whole
        for i in range(step + 1):
            work = work - combine(found[i], basis[i])
            block = block - jnp.dot(found[i], found[i].T, precision=lax.Precision.HIGHEST)
        lower = jnp.linalg.cholesky(block)
        basis.append(lower_solve(lower, work))
        coefs.append(found)
        lowers.append(lower)
    mix, hess, target = small_solve(coefs, lowers, lead)
    combo = combine(mix[:, :S], basis[0])
    for j in range(1, ITERS):
        combo = combo + combine(mix[:, j * S : (j + 1) * S], basis[j])
    solution = precondition(combo, operate, inv_diag)
    residual = start - operate(solution)
    return (solution, residual)

LANES = 128


def full(dims, left, right):
    return lax.dot_general(
        left,
        right,
        (dims, ((), ())),
        precision=lax.Precision.HIGHEST,
        preferred_element_type=jnp.float32,
    )


def chebyshev_steps():
    theta = 0.5 * (cheb_high + cheb_low)
    delta = 0.5 * (cheb_high - cheb_low)
    sigma = theta / delta
    rho = 1.0 / sigma
    steps = []
    for _ in range(DEG - 1):
        rho_next = 1.0 / (2.0 * sigma - rho)
        steps.append((rho_next * rho, 2.0 * rho_next / delta))
        rho = rho_next
    return 1.0 / theta, steps


def spread_rows(value, k):
    return jnp.broadcast_to(value[k : k + 1, :], value.shape)


def spread_lane(value, k):
    return jnp.broadcast_to(value[:, k : k + 1], value.shape)


def times(columns, block):
    total = columns[0] * spread_rows(block, 0)
    for c in range(1, 8):
        total = total + columns[c] * spread_rows(block, c)
    return total


def invert(cols, row):
    cols = list(cols)
    for k in range(8):
        over = 1.0 / spread_rows(cols[k], k)
        pivot = cols[k]
        for c in range(8):
            if c == k:
                cols[c] = jnp.where(row == k, over, -pivot * over)
            else:
                scaled = spread_rows(cols[c], k) * over
                cols[c] = jnp.where(row == k, scaled, cols[c] - pivot * scaled)
    return cols


def block_jordan(blocks, row):
    blocks = list(blocks)
    for k in range(len(blocks)):
        cols = [[spread_lane(b, 8 * k + c) for c in range(8)] for b in blocks]
        solved = times(invert(cols[k], row), blocks[k])
        for i in range(len(blocks)):
            blocks[i] = solved if i == k else blocks[i] - times(cols[i], solved)
    return blocks


SPREAD = 0.52
REACH = 2


def kernel(
    dims,
    rhs_hbm, perm_hbm, accum_hbm, counts_hbm, out0_ref, out1_ref,
    rhs_ref, perm_ref, accum_ref, counts_ref, load_sem,
    pick_ref, ends_ref, raw_ref, out_ref, flux_ref, in_buf, in_got, out_buf, out_got, rim_buf, rim_got,
    wall, edge_ref,
    ext, coef, inv, diag_own, first_field, basis, big, found, d1, d2, d3, rem,
    part, got1, mid, got2, square,
    in_send, in_recv, out_send, out_recv, xs_send, xs_recv, halo_send, halo_recv, s1_send, s1_recv, s2_send, s2_recv,
):
    nsub, nslab, zl, yl_n, pack, nx = dims
    halo = DEG * REACH
    pad = halo + 1
    span = zl + 2 * halo
    per = yl_n + 1
    sub = lax.axis_index("sub")
    slab = lax.axis_index("slab")

    total = nsub * nslab
    layer, core = slab // 2, lax.rem(slab, 2)
    at = sub // 2 + lax.rem(sub, 2) * (nsub - 1 - 2 * (sub // 2))
    at = at + lax.rem(layer, 2) * (nsub - 1 - 2 * at)
    place = 2 * (layer * nsub + at) + core
    home, mine = place // nsub, lax.rem(place, nsub)
    nxt = lax.rem(place + 1, total)
    prv = lax.rem(place + total - 1, total)

    def dev(g):
        chip = g // 2
        layer = chip // nsub
        at = lax.rem(chip, nsub)
        at = at + lax.rem(layer, 2) * (nsub - 1 - 2 * at)
        across = at // (nsub // 2)
        return {"sub": 2 * (at + across * (nsub - 1 - 2 * at)) + across, "slab": 2 * layer + lax.rem(g, 2)}

    loads = [
        pltpu.make_async_copy(src, dst, load_sem.at[k])
        for k, (src, dst) in enumerate(
            ((perm_hbm, perm_ref), (accum_hbm, accum_ref), (rhs_hbm, rhs_ref), (counts_hbm, counts_ref))
        )
    ]
    for c in loads:
        c.start()

    barrier = pltpu.get_barrier_semaphore()
    peers = [{"slab": lax.rem(slab + d, nslab)} for d in range(1, nslab)]
    for d in range(1, nsub):
        peers += [{"sub": lax.rem(sub + d, nsub)}, {"sub": lax.rem(sub + d, nsub), "slab": 2 * layer + 1 - core}]
    for device in peers:
        pl.semaphore_signal(barrier, inc=1, device_id=device, device_id_type=pl.DeviceIdType.MESH)

    def remote(src, dst, send, recv, device):
        return pltpu.make_async_remote_copy(
            src_ref=src, dst_ref=dst, send_sem=send, recv_sem=recv,
            device_id=device, device_id_type=pl.DeviceIdType.MESH,
        )

    group = pack * (LANES // (pack * nsub))
    square[...] = jnp.zeros_like(square)
    for c in loads:
        c.wait()
    pieces = [ref[pl.ds(y, group, stride=yl_n), :] for ref in (perm_ref, accum_ref) for y in range(yl_n)]
    in_buf[yl_n] = jnp.concatenate(pieces, axis=0).T
    for y in range(yl_n):
        in_buf[y] = rhs_ref[pl.ds(y, LANES, stride=yl_n), :].T

    pl.semaphore_wait(barrier, len(peers))

    def rows_of(i):
        return pl.ds(pl.multiple_of(i * zl, 8), zl)

    halves = ((yl_n, 1), (0, yl_n))
    flip = jnp.where(sub // 2 < nsub // 4, 1, 0)

    def far_first(k):
        return k // 2 + flip * (nsub // 2 - 1 - 2 * (k // 2))

    arrivals = []
    for k, (t, n) in enumerate(halves):
        for d in range(nsub):
            deep = far_first(d)
            q = 2 * (deep + lax.rem(slab, 2) * (nsub // 2 - 1 - 2 * deep)) + d % 2
            goal = slab * nsub + q
            c = remote(
                in_buf.at[t : t + n, rows_of(q), :], in_got.at[sub, t : t + n],
                in_send.at[k, d], in_recv.at[k, sub], dev(goal),
            )
            pl.when(goal != place)(c.start)
            arrivals.append((goal != place, c))

    @pl.when(home == slab)
    def _():
        in_got[sub] = in_buf[:, rows_of(mine), :]

    def arrived(k):
        t, n = halves[k]
        for i in range(nsub):
            c = remote(
                in_buf.at[t : t + n, 0:zl, :], in_got.at[i, t : t + n],
                in_send.at[k, i], in_recv.at[k, i], {"sub": i, "slab": home},
            )
            pl.when((home != slab) | (sub != i))(c.wait_recv)

    wide_row = lax.broadcasted_iota(jnp.int32, (LANES, LANES), 0)
    wide_lane = lax.broadcasted_iota(jnp.int32, (LANES, LANES), 1)
    rank = lax.rem(wide_row, group) // pack
    owner = wide_row // group
    base_of = jnp.zeros_like(wide_row)
    live_of = jnp.zeros_like(wide_row)
    before = jnp.int32(0)
    for i in range(nsub):
        live = counts_ref[i]
        base_of = jnp.where(owner == i, before, base_of)
        live_of = jnp.where(owner == i, live, live_of)
        before = before + live
    goal = base_of + rank + lax.rem(wide_row, pack) * nx
    pick_ref[...] = jnp.where((rank < live_of) & (goal == wide_lane), 1.0, 0.0).astype(jnp.float32)

    owner = wide_lane // group
    target = jnp.zeros_like(wide_row)
    before = jnp.int32(0)
    for i in range(nsub):
        face = before - 1 + lax.rem(wide_lane // 8, 2) * counts_ref[i]
        target = jnp.where(owner == i, face, target)
        before = before + counts_ref[i]
    at_face = (lax.rem(wide_row, nx) == target) & (wide_row // nx == lax.rem(wide_lane // yl_n, 2))
    for y in range(yl_n):
        ends_ref[y] = jnp.where(at_face & (lax.rem(wide_lane, yl_n) == y), 1.0, 0.0).astype(jnp.float32)

    live_here = counts_ref[sub]
    depth = perm_ref.shape[0] // 8

    def plane(p):
        return slice(8 * p, 8 * p + 8)

    tall = lax.broadcasted_iota(jnp.int32, (8, LANES), 0)
    long = lax.broadcasted_iota(jnp.int32, (8, LANES), 1)
    for p in range(depth):
        mine_perm = perm_ref[plane(p), :]
        alive = jnp.where(p < live_here, 2.0, 0.0).astype(jnp.float32)
        if p + 1 < depth:
            other = perm_ref[plane(p + 1), :]
            joined = jnp.where(p + 1 < live_here, 2.0, 0.0).astype(jnp.float32)
            wall[0, plane(p), :] = joined * mine_perm * other / (mine_perm + other)
        other = pltpu.roll(mine_perm, 7, 0)
        wall[1, plane(p), :] = jnp.where(tall < 7, alive * mine_perm * other / (mine_perm + other), 0.0)
        other = pltpu.roll(mine_perm, LANES - 1, 1)
        wall[2, plane(p), :] = jnp.where(long < LANES - 1, alive * mine_perm * other / (mine_perm + other), 0.0)

    strip = lax.broadcasted_iota(jnp.int32, (zl, LANES), 1) // group

    def butterfly(items):
        d = len(items) // 2
        while d:
            fresh = list(items)
            for a in range(len(items)):
                if a & d:
                    continue
                first_half = (strip[0 : items[a].shape[0], :] & d) == 0
                fresh[a] = jnp.where(first_half, items[a], pltpu.roll(items[a + d], group * d, 1))
                fresh[a + d] = jnp.where(first_half, pltpu.roll(items[a], LANES - group * d, 1), items[a + d])
            items = fresh
            d //= 2
        return items

    lane = lax.broadcasted_iota(jnp.int32, (8, LANES), 1)
    row = lax.broadcasted_iota(jnp.int32, (8, LANES), 0)
    tile = yl_n * LANES
    side = halo * tile
    own_lo, own_hi = side, side + zl * tile

    arrived(0)
    for i, value in enumerate(butterfly([in_got[i, yl_n] for i in range(nsub)])):
        raw_ref[pl.ds(i, zl, stride=8), :] = value
    packed = full(((1,), (0,)), raw_ref[0 : zl * 8, :], pick_ref[...])
    for k in range(zl):
        at = (pad + k) * LANES
        ext[:, at : at + LANES] = packed[k * 8 : k * 8 + 8, :]
    edge = pad * LANES
    whole = zl * LANES
    up = remote(ext.at[:, whole : whole + edge], ext.at[:, 0:edge], xs_send.at[0], xs_recv.at[0], dev(nxt))
    down = remote(ext.at[:, edge : 2 * edge], ext.at[:, edge + whole : 2 * edge + whole], xs_send.at[1], xs_recv.at[1], dev(prv))
    up.start()
    down.start()

    along = lax.rem(lane, nx)

    def fill(e, _):
        def grab(t):
            return ext[:, pl.ds(pl.multiple_of((e + 1 + t) * LANES, LANES), LANES)]

        here, after, before = grab(0), grab(1), grab(-1)
        swap_up = jnp.where(lane >= LANES - nx, 0.0, pltpu.roll(here, LANES - nx, 1))
        swap_down = jnp.where(lane < nx, 0.0, pltpu.roll(here, nx, 1))
        others = (
            jnp.where(along == nx - 1, 0.0, pltpu.roll(here, LANES - 1, 1)),
            jnp.where(along == 0, 0.0, pltpu.roll(here, 1, 1)),
            jnp.where(row == yl_n - 1, pltpu.roll(swap_up, yl_n - 1, 0), pltpu.roll(here, 7, 0)),
            jnp.where(row == 0, pltpu.roll(swap_down, 8 - (yl_n - 1), 0), pltpu.roll(here, 1, 0)),
            after,
            before,
        )
        diag = pltpu.roll(here, 8 - yl_n, 0)
        weights = []
        for q in others:
            both = here * q
            weight = jnp.where(both > 0.0, 2.0 * both / jnp.where(both > 0.0, here + q, 1.0), 0.0)
            weights.append(weight)
            diag = diag + weight
        over = jnp.where(diag > 0.0, 1.0 / jnp.where(diag > 0.0, diag, 1.0), 0.0)
        weights = [weight * over for weight in weights]
        for y in range(yl_n):
            at = pl.ds(pl.multiple_of((e * yl_n + y) * LANES, LANES), LANES)
            for k, weight in enumerate(weights):
                coef[k, :, at] = spread_rows(weight, y)
            inv[:, at] = spread_rows(over, y)
            diag_own[:, at] = spread_rows(diag, y)
        return 0

    lax.fori_loop(halo + 1, halo + zl - 1, fill, 0)

    arrived(1)
    for t in range(yl_n):
        for i, value in enumerate(butterfly([in_got[i, t] for i in range(nsub)])):
            raw_ref[pl.ds(t * 8 + i, zl, stride=yl_n * 8), :] = value
    packed = full(((1,), (0,)), raw_ref[...], pick_ref[...])
    for k in range(zl * yl_n):
        basis[0, :, own_lo + k * LANES : own_lo + (k + 1) * LANES] = packed[k * 8 : k * 8 + 8, :]
        big[0:8, k * LANES : (k + 1) * LANES] = packed[k * 8 : k * 8 + 8, :]

    def swap(n, m):
        return [
            remote(
                basis.at[n, :, own_hi - side : own_hi], basis.at[n, :, 0:side],
                halo_send.at[m, 0], halo_recv.at[m, 0], dev(nxt),
            ),
            remote(
                basis.at[n, :, own_lo : own_lo + side], basis.at[n, :, own_hi : own_hi + side],
                halo_send.at[m, 1], halo_recv.at[m, 1], dev(prv),
            ),
        ]

    first_swap = swap(0, 0)
    for c in first_swap:
        c.start()

    def products(j):
        blocks = j + 1

        def add(k, accs):
            accs = list(accs)
            for h in range(4):
                at = pl.ds(pl.multiple_of((4 * k + h) * LANES, LANES), LANES)
                w = big[8 * j : 8 * j + 8, at]
                turned = [w] + [pltpu.roll(w, n, 0) for n in range(1, 8)]
                for b in range(blocks):
                    v = w if b == j else big[8 * b : 8 * b + 8, at]
                    for n in range(8):
                        accs[8 * b + n] = accs[8 * b + n] + v * turned[n]
            return tuple(accs)

        zero = jnp.zeros((8, LANES), jnp.float32)
        accs = lax.fori_loop(0, zl * yl_n // 4, add, (zero,) * (8 * blocks))
        out = zero
        for b in range(blocks):
            for n in range(8):
                acc = accs[8 * b + n]
                acc = pltpu.roll(acc, 8 - n, 0) if n else acc
                line = jnp.sum(acc, axis=1, keepdims=True)
                out = jnp.where(lane == 8 * b + lax.rem(row + n, 8), line, out)
        return out

    sends = []

    def reduce_begin(r, gram):
        part[r] = gram
        got1[r, slab] = part[r]
        for d in range(1, nslab):
            peer = lax.rem(slab + d, nslab)
            c = remote(part.at[r], got1.at[r, slab], s1_send.at[r, d], s1_recv.at[r, slab], {"slab": peer})
            c.start()
            sends.append(c)

    def reduce_middle(r):
        for d in range(1, nslab):
            peer = lax.rem(slab + d, nslab)
            remote(part.at[r], got1.at[r, peer], s1_send.at[r, d], s1_recv.at[r, peer], {"slab": peer}).wait_recv()
        acc = got1[r, 0]
        for i in range(1, nslab):
            acc = acc + got1[r, i]
        mid[r] = acc
        got2[r, sub] = acc
        for d in range(1, nsub):
            peer = lax.rem(sub + d, nsub)
            c = remote(mid.at[r], got2.at[r, sub], s2_send.at[r, d], s2_recv.at[r, sub], {"sub": peer})
            c.start()
            sends.append(c)

    def reduce_end(r):
        for d in range(1, nsub):
            peer = lax.rem(sub + d, nsub)
            remote(mid.at[r], got2.at[r, peer], s2_send.at[r, d], s2_recv.at[r, peer], {"sub": peer}).wait_recv()
        acc = got2[r, 0]
        for i in range(1, nsub):
            acc = acc + got2[r, i]
        return acc

    up.wait()
    down.wait()
    low = jnp.where(place == 0, 0.0, 1.0).astype(jnp.float32)
    high = jnp.where(place == total - 1, 0.0, 1.0).astype(jnp.float32)
    for k in range(pad):
        a = k * LANES
        ext[:, a : a + LANES] = ext[:, a : a + LANES] * low
        b = (pad + zl + k) * LANES
        ext[:, b : b + LANES] = ext[:, b : b + LANES] * high
    lax.fori_loop(0, halo + 1, fill, 0)
    lax.fori_loop(halo + zl - 1, span, fill, 0)

    def scale(lo, hi):
        for k in range(lo * yl_n, hi * yl_n):
            at = slice(k * LANES, (k + 1) * LANES)
            first_field[:, at] = basis[0, :, at] * inv[:, at]

    scale(halo, halo + zl)

    first, steps = chebyshev_steps()

    def spot(e, y):
        if isinstance(e, int):
            return pl.ds((e * yl_n + y) * LANES, LANES)
        return pl.ds(pl.multiple_of((e * yl_n + y) * LANES, LANES), LANES)

    def beside(field, e):
        here = [field[:, spot(e, y)] for y in range(yl_n)]
        outs = []
        for y in range(yl_n):
            at = spot(e, y)
            f = here[y]
            y_up = here[y + 1] if y + 1 < yl_n else pltpu.roll(here[0], LANES - nx, 1)
            y_down = here[y - 1] if y > 0 else pltpu.roll(here[yl_n - 1], nx, 1)
            acc = coef[0, :, at] * pltpu.roll(f, LANES - 1, 1)
            acc = acc + coef[1, :, at] * pltpu.roll(f, 1, 1)
            acc = acc + coef[2, :, at] * y_up
            acc = acc + coef[3, :, at] * y_down
            acc = acc + coef[4, :, at] * field[:, spot(e + 1, y)]
            acc = acc + coef[5, :, at] * field[:, spot(e - 1, y)]
            outs.append(acc)
        return here, outs

    def field_of(j):
        return first_field if j == 0 else basis.at[j]

    def advance(j, t, planes):
        fields = (field_of(j), d1, d2, d3)
        source = fields[t]
        for e in planes:
            here, outs = beside(source, e)
            for y in range(yl_n):
                at = spot(e, y)
                if t < DEG - 1:
                    keep, gain = steps[t]
                    if t == 0:
                        r = here[y] - first * (here[y] - outs[y])
                        d = (keep * first) * here[y] + gain * r
                    else:
                        r = rem[:, at] - here[y] + outs[y]
                        d = keep * here[y] + gain * r
                    rem[:, at] = r
                    fields[t + 1][:, at] = d
                    continue
                r = rem[:, at] - here[y] + outs[y]
                value = r * (1.0 / SPREAD) if j == 0 else r * (2.0 / SPREAD) - field_of(j - 1)[:, at]
                if j + 1 < ITERS:
                    basis[j + 1, :, at] = value
                if halo <= e < halo + zl:
                    big[8 * (j + 1) : 8 * (j + 2), spot(e - halo, y)] = value * diag_own[:, at]
                if halo - 1 <= e <= halo + zl:
                    found[8 * j : 8 * (j + 1), spot(e - halo + 1, y)] = first * fields[0][:, at] + d1[:, at] + d2[:, at] + here[y]

    moves = first_swap
    for j in range(ITERS):
        inset = DEG * (j % REACH)
        if not inset:
            for t in range(DEG):
                advance(j, t, range(halo + t + 1, halo + zl - t - 1))
            reduce_begin(j, products(j))
            for c in moves:
                c.wait()
            if not j:
                scale(0, halo)
                scale(halo + zl, span)
            for t in range(DEG):
                outer = [*range(t + 1, halo + t + 1), *range(halo + zl - t - 1, span - t - 1)]
                advance(j, t, outer)
        else:
            for t in range(DEG):
                advance(j, t, range(inset + t + 1, span - inset - t - 1))
            for e in (halo - 1, halo + zl):
                for y in range(yl_n):
                    at = spot(e, y)
                    found[8 * j : 8 * (j + 1), spot(e - halo + 1, y)] = (
                        first * field_of(j)[:, at] + d1[:, at] + d2[:, at] + d3[:, at]
                    )
        if (j + 1) % REACH == 0 and j + 1 < ITERS:
            moves = swap(j + 1, (j + 1) // REACH)
            for c in moves:
                c.start()
        else:
            reduce_begin(j + 1, products(j + 1))
        if j == 2:
            for r in range(3):
                reduce_middle(r)
    for r in range(3, ITERS + 1):
        reduce_middle(r)

    rows = 8 * ITERS
    for r in range(ITERS + 1):
        square[8 * r : 8 * r + 8, :] = reduce_end(r)
    turned = square[...].T
    gram = [
        jnp.where(lane < 8 * (r + 1), square[8 * r : 8 * r + 8, :], turned[8 * r : 8 * r + 8, :])
        for r in range(ITERS + 1)
    ]
    up_by = jnp.where(lane < 8, SPREAD, 0.5 * SPREAD)
    down_by = jnp.where(lane < 8, 0.0, 0.5 * SPREAD)
    system = []
    for j in range(ITERS):
        mixed = gram[j] - SPREAD * gram[1] if j == 0 else gram[j] - (0.5 * SPREAD) * (gram[j + 1] + gram[j - 1])
        both = mixed - up_by * pltpu.roll(mixed, LANES - 8, 1) - down_by * pltpu.roll(mixed, 8, 1)
        right = pltpu.roll(mixed, rows, 1)
        system.append(jnp.where(lane < rows, both, jnp.where(lane < rows + 8, right, 0.0)))
    solved = block_jordan(system, row)
    filled = jnp.concatenate([*solved, jnp.zeros((LANES - rows, LANES), jnp.float32)], axis=0)
    mix = filled.T[rows : rows + 8, :]
    leaving = []
    half = zl // 2
    capped = (mine == 0) | (mine == nsub - 1)

    def part_of(f, q, peer):
        if f < 2:
            rows_at = pl.ds(pl.multiple_of(q * zl + f * half, 8), half)
            return out_buf.at[peer, :, f * half : (f + 1) * half, :], out_got.at[:, rows_at, :]
        if f == 2:
            return rim_buf.at[peer, 0:zl], rim_got.at[q, 0:zl]
        return rim_buf.at[peer, zl : zl + 8], rim_got.at[q, zl : zl + 8]

    def send(f):
        for d in range(nsub):
            peer = 2 * far_first(d) + d % 2
            src, dst = part_of(f, mine, peer)
            c = remote(src, dst, out_send.at[f, d], out_recv.at[f, mine], {"sub": peer, "slab": home})
            away = (home != slab) | (peer != sub)
            if f == 3:
                away = away & capped
            pl.when(away)(c.start)
            leaving.append((away, c))

    def landed(f):
        for q in range(nsub) if f < 3 else (0, nsub - 1):
            src, dst = part_of(f, q, 0)
            c = remote(src, dst, out_send.at[f, q], out_recv.at[f, q], dev(slab * nsub + q))
            pl.when(slab * nsub + q != place)(c.wait_recv)

    pieces = []
    for f in range(2):
        lo = (f * (half + 1)) * yl_n * LANES
        hi = lo + (half + 1) * yl_n * LANES
        piece = full(((1,), (0,)), mix[:, 0:rows], found[:, lo:hi])
        pieces.append(piece)
        for e in range(f * half, (f + 1) * half):
            for y in range(yl_n):
                k = (e + 1) * yl_n + y
                at = k * LANES - lo
                k = e * yl_n + y
                if f == 0 or at + LANES <= hi - lo:
                    out_ref[k * 8 : k * 8 + 8, :] = piece[:, at : at + LANES]
        base = f * half * yl_n * 8
        raw_ref[base : base + half * yl_n * 8, :] = full(
            ((1,), (1,)), out_ref[base : base + half * yl_n * 8, :], pick_ref[...]
        )
        for y in range(yl_n):
            items = [raw_ref[pl.ds(base + y * 8 + i, half, stride=yl_n * 8), :] for i in range(nsub)]
            for i, value in enumerate(butterfly(items)):
                out_buf[i, y, f * half : (f + 1) * half, :] = value
        send(f)

    def sol_at(e, y):
        k = (e + 1) * yl_n + y
        f = k // ((half + 1) * yl_n)
        at = (k - f * (half + 1) * yl_n) * LANES
        return pieces[f][:, at : at + LANES]

    @pl.when(home == slab)
    def _():
        out_got[:, rows_of(mine), :] = out_buf[sub]

    for e in range(zl):
        for y in range(yl_n):
            at = spot(halo + e, y)
            k = e * yl_n + y
            value = out_ref[k * 8 : k * 8 + 8, :]
            drop = value - pltpu.roll(value, LANES - 1, 1)
            flux_ref[y, e * 8 : e * 8 + 8, :] = coef[0, :, at] * diag_own[:, at] * drop
    faces = full(((1,), (0,)), flux_ref[0], ends_ref[0])
    for y in range(1, yl_n):
        faces = faces + full(((1,), (0,)), flux_ref[y], ends_ref[y])
    for y in range(yl_n):
        at = spot(halo, y)
        flux_ref[0, y * 8 : y * 8 + 8, :] = coef[5, :, at] * diag_own[:, at] * (sol_at(-1, y) - sol_at(0, y))
        at = spot(halo + zl - 1, y)
        flux_ref[1, y * 8 : y * 8 + 8, :] = coef[4, :, at] * diag_own[:, at] * (sol_at(zl - 1, y) - sol_at(zl, y))
    raw_ref[0 : zl * 8, :] = faces
    for f in range(2):
        raw_ref[zl * 8 + f * yl_n * 8 : zl * 8 + (f + 1) * yl_n * 8, :] = full(
            ((1,), (1,)), flux_ref[f, 0 : yl_n * 8, :], pick_ref[...]
        )
    for i, value in enumerate(butterfly([raw_ref[pl.ds(i, zl, stride=8), :] for i in range(nsub)])):
        rim_buf[i, 0:zl, :] = value
    send(2)
    for i, value in enumerate(butterfly([raw_ref[pl.ds(zl * 8 + i, 8, stride=8), :] for i in range(nsub)])):
        rim_buf[i, zl : zl + 8, :] = value
    send(3)

    @pl.when(home == slab)
    def _():
        rim_got[mine] = rim_buf[sub]

    landed(0)
    landed(1)
    for y in range(yl_n):
        out0_ref[pl.ds(y, LANES, stride=yl_n), :] = out_got[y].T
    landed(2)
    landed(3)
    around = jnp.concatenate([rim_got[q, 0:zl, :] for q in range(nsub)], axis=0).T
    caps = jnp.concatenate(
        [rim_got[0, zl : zl + yl_n, :], rim_got[nsub - 1, zl + yl_n : zl + 8, :], jnp.zeros((LANES - 8, LANES), jnp.float32)],
        axis=0,
    ).T
    for y in range(yl_n):
        lower = jnp.broadcast_to(caps[:, y : y + 1], (LANES, LANES))
        upper = jnp.broadcast_to(caps[:, yl_n + y : yl_n + y + 1], (LANES, LANES))
        edge_ref[pl.ds(y, LANES, stride=yl_n), :] = jnp.where(
            wide_lane == 0, lower, jnp.where(wide_lane == LANES - 1, -upper, 0.0)
        )
    for i in range(8):
        def rows_at(p):
            return slice((i * depth + p) * 8, (i * depth + p + 1) * 8)

        carried = around[16 * i : 16 * i + 8, :]
        beyond = around[16 * i + 8 : 16 * i + 16, :]
        value = out0_ref[rows_at(0), :]
        for p in range(depth):
            alive = jnp.where(p < live_here, 1.0, 0.0).astype(jnp.float32)
            final = jnp.where(p + 1 == live_here, 1.0, 0.0).astype(jnp.float32)
            rest = alive * rhs_ref[rows_at(p), :] + edge_ref[rows_at(p), :] - accum_ref[plane(p), :] * value
            rest = rest + carried - final * beyond
            fy = wall[1, plane(p), :] * (value - pltpu.roll(value, 7, 0))
            fz = wall[2, plane(p), :] * (value - pltpu.roll(value, LANES - 1, 1))
            rest = rest - (fy - pltpu.roll(fy, 1, 0)) - (fz - pltpu.roll(fz, 1, 1))
            if p + 1 < depth:
                ahead = out0_ref[rows_at(p + 1), :]
                carried = wall[0, plane(p), :] * (value - ahead)
                rest = rest - carried
                value = ahead
            out1_ref[rows_at(p), :] = rest
    for away, c in arrivals + leaving:
        pl.when(away)(c.wait_send)
    for c in sends:
        c.wait_send()


def fast_body(rhs, perm, accum, counts):
    nsub, nslab = lax.axis_size("sub"), lax.axis_size("slab")
    s, depth, cy, zs = rhs.shape
    nx = depth * nsub
    pack = LANES // nx
    yl = cy // pack
    zl = zs // nsub
    halo = DEG * REACH
    span = zl + 2 * halo
    pad = halo + 1

    wide = span * yl * LANES
    own = zl * yl * LANES
    f32 = jnp.float32
    rounds = ITERS + 1
    dma = pltpu.SemaphoreType.DMA
    out = pl.pallas_call(
        functools.partial(kernel, (nsub, nslab, zl, yl, pack, nx)),
        out_shape=[jax.ShapeDtypeStruct((s * depth * cy, zs), f32)] * 2,
        in_specs=[pl.BlockSpec(memory_space=pltpu.HBM)] * 4,
        out_specs=[pl.BlockSpec(memory_space=pltpu.VMEM)] * 2,
        scratch_shapes=[
            pltpu.VMEM((s * depth * cy, zs), f32),
            pltpu.VMEM((depth * cy, zs), f32),
            pltpu.VMEM((depth * cy, zs), f32),
            pltpu.SMEM((nsub,), jnp.int32),
            dma((4,)),
            pltpu.VMEM((LANES, LANES), f32),
            pltpu.VMEM((yl, LANES, LANES), f32),
            pltpu.VMEM((zl * yl * s, LANES), f32),
            pltpu.VMEM((zl * yl * s, LANES), f32),
            pltpu.VMEM((yl, zl * s, LANES), f32),
            pltpu.VMEM((yl + 1, zs, LANES), f32),
            pltpu.VMEM((nsub, yl + 1, zl, LANES), f32),
            pltpu.VMEM((nsub, yl, zl, LANES), f32),
            pltpu.VMEM((yl, zs, LANES), f32),
            pltpu.VMEM((nsub, zl + 8, LANES), f32),
            pltpu.VMEM((nsub, zl + 8, LANES), f32),
            pltpu.VMEM((3, depth * cy, zs), f32),
            pltpu.VMEM((s * depth * cy, zs), f32),
            pltpu.VMEM((8, (zl + 2 * pad) * LANES), f32),
            pltpu.VMEM((6, 8, wide), f32),
            pltpu.VMEM((8, wide), f32),
            pltpu.VMEM((8, wide), f32),
            pltpu.VMEM((8, wide), f32),
            pltpu.VMEM((ITERS, 8, wide), f32),
            pltpu.VMEM((8 * rounds, own), f32),
            pltpu.VMEM((8 * ITERS, own + 2 * yl * LANES), f32),
            pltpu.VMEM((8, wide), f32),
            pltpu.VMEM((8, wide), f32),
            pltpu.VMEM((8, wide), f32),
            pltpu.VMEM((8, wide), f32),
            pltpu.VMEM((rounds, 8, LANES), f32),
            pltpu.VMEM((rounds, nslab, 8, LANES), f32),
            pltpu.VMEM((rounds, 8, LANES), f32),
            pltpu.VMEM((rounds, nsub, 8, LANES), f32),
            pltpu.VMEM((LANES, LANES), f32),
            dma((2, nsub)),
            dma((2, nsub)),
            dma((4, nsub)),
            dma((4, nsub)),
            dma((2,)),
            dma((2,)),
            dma((ITERS // REACH, 2)),
            dma((ITERS // REACH, 2)),
            dma((rounds, nslab)),
            dma((rounds, nslab)),
            dma((rounds, nsub)),
            dma((rounds, nsub)),
        ],
        compiler_params=pltpu.CompilerParams(
            collective_id=0, has_side_effects=True, vmem_limit_bytes=60*1024*1024
        ),
    )(rhs.reshape(-1, zs), perm.reshape(-1, zs), accum.reshape(-1, zs), counts)
    return out[0].reshape(rhs.shape), out[1].reshape(rhs.shape)


def choose(rhs, perm, accum, counts):
    nsub = lax.axis_size("sub")
    s, depth, cy, zs = rhs.shape
    nx = depth * nsub
    fits = s == S == nsub == 8 and zs == LANES and depth == cy == 8 and zs // nsub % 8 == 0 and LANES % nx == 0 and zs % nsub == 0 and lax.axis_size("slab") % 2 == 0 and zs // nsub > DEG * REACH
    fits = fits and cy % max(LANES // nx, 1) == 0 and cy // max(LANES // nx, 1) == 4
    if fits:
        return fast_body(rhs, perm, accum, counts)
    return body(rhs, perm, accum, counts)


def solution(mesh):
    placed = (P(None, "sub", None, "slab"), P("sub", None, "slab"), P("sub", None, "slab"), P())
    return jax.shard_map(
        choose,
        mesh=mesh,
        in_specs=placed,
        out_specs=(P(None, "sub", None, "slab"), P(None, "sub", None, "slab")),
        check_vma=False,
    )
```
